32 devices in a mesh: dp: 2 (over x), tp: 4 (over z), ep: 4 (over y, core).
Axes of the slice: x: 2, y: 2, z: 4, core: 2. Of those that a mesh axis runs over, the one named last changes fastest.
Arguments:
- x: bfloat16 [2048, 2048], P(('dp', 'tp', 'ep')), parts along dimension 0
- route_idx: int32 [2048, 8], P(('dp', 'tp', 'ep')), parts along dimension 0
- gates: float32 [2048, 8], P(('dp', 'tp', 'ep')), parts along dimension 0
- w1: bfloat16 [64, 2048, 1024], P('ep', None, 'tp')
- w3: bfloat16 [64, 2048, 1024], P('ep', None, 'tp')
- w2: bfloat16 [64, 1024, 2048], P('ep', 'tp')
Outputs:
- output: bfloat16 [2048, 2048], P(('dp', 'tp', 'ep')), parts along dimension 0
There are 2 independent parts. The reference program is written for one: setup_inputs(seed, part) draws one part's arguments, and reference() takes and returns one part's arrays. A program takes and returns all parts, laid end to end along the dimension named above; an argument that names none is the same for every part.
All inputs are finite; a program needn't handle non-finite values.
Results may differ from the reference program's by a relative error of at most 0.00782163.
Values are sent between devices in bfloat16 or wider.
A program may use at most 1 GiB of HBM per device.

```python
import jax
import jax.numpy as jnp
from jax import lax

D = 2048
E = 64
F = 1024
TOP = 8
T_LOC = 64
GROUP = 16
N_TOK = GROUP * T_LOC
CAP = T_LOC // 2


def device_routes(key, z):
    kn, kp, ks = jax.random.split(key, 3)
    q = jax.nn.softmax(z + 0.5 * jax.random.normal(kn, (E,), jnp.float32))
    lim = (CAP - 2) / (TOP * T_LOC)
    p1 = jnp.minimum(q, lim)
    room = lim - p1
    p = p1 + (1.0 - jnp.sum(p1)) * room / jnp.maximum(jnp.sum(room), 1e-9)
    total = TOP * T_LOC
    bounds = jnp.floor(total * jnp.cumsum(p)[:-1]).astype(jnp.int32)
    ids = jnp.sum((jnp.arange(total)[:, None] >= bounds[None, :]).astype(jnp.int32), axis=1)
    route = ids.reshape(TOP, T_LOC).T
    route = route[jax.random.permutation(kp, T_LOC)]
    order = jnp.argsort(jax.random.uniform(ks, (T_LOC, TOP), jnp.float32), axis=1)
    return jnp.take_along_axis(route, order, axis=1).astype(jnp.int32)


def setup_inputs(seed: int = 0, part: int = 0) -> dict:
    kpart = jax.random.fold_in(jax.random.key(seed), part)
    kx, kr, kg, kh = jax.random.split(kpart, 4)
    k1, k3, k2 = jax.random.split(jax.random.key(seed + 1), 3)
    x = jax.random.normal(kx, (N_TOK, D), jnp.float32).astype(jnp.bfloat16)
    hot = 1.5 * jax.random.normal(kh, (E,), jnp.float32)
    route_idx = jax.vmap(lambda k: device_routes(k, hot))(jax.random.split(kr, GROUP)).reshape(N_TOK, TOP)
    gates = jax.random.uniform(kg, (N_TOK, TOP), jnp.float32, 0.5, 1.5) * TOP ** -0.5
    w1 = (jax.random.normal(k1, (E, D, F), jnp.float32) * D ** -0.5).astype(jnp.bfloat16)
    w3 = (jax.random.normal(k3, (E, D, F), jnp.float32) * D ** -0.5).astype(jnp.bfloat16)
    w2 = (jax.random.normal(k2, (E, F, D), jnp.float32) * F ** -0.5).astype(jnp.bfloat16)
    return {'x': x, 'route_idx': route_idx, 'gates': gates, 'w1': w1, 'w3': w3, 'w2': w2}


def reference(x, route_idx, gates, w1, w3, w2):
    n_tok = x.shape[0]
    cap_e = n_tok // 2
    xp = jnp.concatenate([x, jnp.zeros((1, D), x.dtype)], axis=0)
    tok = jnp.arange(n_tok, dtype=jnp.int32)

    def body(acc, inp):
        e, a1, a3, a2 = inp
        sel = route_idx == e
        wt = jnp.sum(jnp.where(sel, gates, 0.0), axis=1)
        m = jnp.any(sel, axis=1)
        pos = jnp.where(m, jnp.cumsum(m.astype(jnp.int32)) - 1, cap_e)
        idx = jnp.full((cap_e,), n_tok, jnp.int32).at[pos].set(tok, mode='drop')
        xs = xp[idx]
        a = jnp.dot(xs, a1, preferred_element_type=jnp.float32)
        b = jnp.dot(xs, a3, preferred_element_type=jnp.float32)
        h = (jax.nn.silu(a) * b).astype(jnp.bfloat16)
        o = jnp.dot(h, a2, preferred_element_type=jnp.float32).astype(jnp.bfloat16)
        op = jnp.concatenate([o, jnp.zeros((1, D), o.dtype)], axis=0)
        return acc + op[pos].astype(jnp.float32) * wt[:, None], None

    acc, _ = lax.scan(body, jnp.zeros((n_tok, D), jnp.float32), (jnp.arange(E, dtype=jnp.int32), w1, w3, w2))
    return acc.astype(jnp.bfloat16)
```

```python
import functools

import jax
import jax.numpy as jnp
from jax import lax
from jax.experimental import pallas as pl
from jax.experimental.pallas import tpu as pltpu
from jax.sharding import PartitionSpec as P

TM = 128
BR = 16
LAG = 2
NS = LAG + 1
NO = NS + 1
TC = 256
SIZES = (640, 768, 896, 1024, 1152, 1280, 1408, 1536, 1792, 2304)
MESH = pl.DeviceIdType.MESH


def expert_kernel(meta, dest, x, w1, w3, w2, out, obuf, cnt, sem):
    e = pl.program_id(0)
    n_tok = x.shape[0]

    def drain(slot):
        def one(_, c):
            pltpu.make_async_copy(obuf.at[slot, pl.ds(0, 8)], out.at[0, pl.ds(0, 8)], sem.at[slot]).wait()
            return c
        lax.fori_loop(0, cnt[slot], one, 0)

    @pl.when(e == 0)
    def _():
        cnt[0] = 0
        cnt[1] = 0
        cnt[2] = 0

    blocks, blocks0, off0, off1 = meta[e, 0], meta[e, 1], meta[e, 2], meta[e, 3]

    def tile(i, c):
        rows = lax.broadcasted_iota(jnp.int32, (TM, n_tok), 0) + i * TM
        pick = jnp.where(dest[0] == rows, 1.0, 0.0).astype(jnp.bfloat16)
        xs = jnp.dot(pick, x[...], preferred_element_type=jnp.float32).astype(jnp.bfloat16)
        a = jnp.dot(xs, w1[0], preferred_element_type=jnp.float32)
        b = jnp.dot(xs, w3[0], preferred_element_type=jnp.float32)
        h = (jax.nn.silu(a) * b).astype(jnp.bfloat16)
        slot = cnt[2]
        drain(slot)
        obuf[slot] = jnp.dot(h, w2[0], preferred_element_type=jnp.float32)
        first = i * (TM // 8)
        n = jnp.minimum(TM // 8, blocks - first)

        def put(k, c):
            g = first + k
            late = g >= blocks0
            half = jnp.where(late, 1, 0)
            to = jnp.where(late, off1 + g - blocks0, off0 + g)
            pltpu.make_async_copy(
                obuf.at[slot, pl.ds(pl.multiple_of(k * 8, 8), 8)],
                out.at[half, pl.ds(pl.multiple_of(to * 8, 8), 8)], sem.at[slot]).start()
            return c

        lax.fori_loop(0, n, put, 0)
        cnt[slot] = n
        cnt[2] = 1 - slot
        return c

    lax.fori_loop(0, (blocks + TM // 8 - 1) // (TM // 8), tile, 0)

    @pl.when(e == pl.num_programs(0) - 1)
    def _():
        drain(0)
        drain(1)


def chain_kernel(n, blocks, src, out, own, rbuf, sbuf, obuf, own_sem, send_sem, recv_sem, out_sem, credit):
    z = lax.axis_index('tp')
    barrier = pltpu.get_barrier_semaphore()

    @pl.when(z > 0)
    def _():
        pl.semaphore_signal(barrier, inc=1, device_id={'tp': z - 1}, device_id_type=MESH)

    @pl.when(z < n - 1)
    def _():
        pl.semaphore_signal(barrier, inc=1, device_id={'tp': z + 1}, device_id_type=MESH)

    pl.semaphore_wait(barrier, jnp.where(z > 0, 1, 0) + jnp.where(z < n - 1, 1, 0))

    def load(d, k):
        s = lax.rem(k, NO)
        return pltpu.make_async_copy(src.at[1 - d, pl.ds(pl.multiple_of(k * BR, BR), BR)], own.at[d, s], own_sem.at[d, s])

    def send(d, k, buf, s_buf):
        s = lax.rem(k, NS)
        to = z + 1 if d == 0 else z - 1
        return pltpu.make_async_remote_copy(
            src_ref=buf.at[d, s_buf], dst_ref=rbuf.at[d, s], send_sem=send_sem.at[d, s], recv_sem=recv_sem.at[d, s],
            device_id={'tp': to}, device_id_type=MESH)

    def put(k):
        s = lax.rem(k, 2)
        return pltpu.make_async_copy(obuf.at[s], out.at[pl.ds(pl.multiple_of(k * BR, BR), BR)], out_sem.at[s])

    def step(i, c):
        work = []
        for d in (0, 1):
            p = z if d == 0 else n - 1 - z
            k = i - LAG * p
            work.append((d, p, k, jnp.logical_and(k >= 0, k < blocks)))

        for d, p, k, live in work:
            @pl.when(live)
            def _(d=d, p=p, k=k):
                @pl.when(jnp.logical_and(p < n - 1, k >= NS))
                def _():
                    send(d, k - NS, sbuf, lax.rem(k, NS)).wait_send()

                @pl.when(k == 0)
                def _():
                    load(d, k).start()

                @pl.when(k + 1 < blocks)
                def _():
                    load(d, k + 1).start()

                load(d, k).wait()

        for d, p, k, live in work:
            @pl.when(jnp.logical_and(live, p == 0))
            def _(d=d, k=k):
                @pl.when(k >= NS)
                def _():
                    pl.semaphore_wait(credit.at[d], 1)
                send(d, k, own, lax.rem(k, NO)).start()

        for d, p, k, live in work:
            @pl.when(jnp.logical_and(live, p > 0))
            def _(d=d, p=p, k=k):
                s = lax.rem(k, NS)
                send(d, k, sbuf, s).wait_recv()

                @pl.when(p < n - 1)
                def _():
                    sbuf[d, s] = rbuf[d, s] + own[d, lax.rem(k, NO)]

                @pl.when(p == n - 1)
                def _():
                    t = lax.rem(k, 2)

                    @pl.when(k >= 2)
                    def _():
                        put(k - 2).wait()
                    obuf[t] = (rbuf[d, s] + own[d, lax.rem(k, NO)]).astype(jnp.bfloat16)
                    put(k).start()

                @pl.when(k + NS < blocks)
                def _():
                    back = z - 1 if d == 0 else z + 1
                    pl.semaphore_signal(credit.at[d], inc=1, device_id={'tp': back}, device_id_type=MESH)

        for d, p, k, live in work:
            @pl.when(jnp.logical_and(live, jnp.logical_and(p > 0, p < n - 1)))
            def _(d=d, k=k):
                @pl.when(k >= NS)
                def _():
                    pl.semaphore_wait(credit.at[d], 1)
                send(d, k, sbuf, lax.rem(k, NS)).start()
        return c

    lax.fori_loop(0, blocks + LAG * (n - 1), step, 0)

    for d in (0, 1):
        p = z if d == 0 else n - 1 - z

        @pl.when(p < n - 1)
        def _(d=d):
            for k in range(blocks - NS, blocks):
                send(d, k, sbuf, k % NS).wait_send()

        @pl.when(p == n - 1)
        def _():
            put(blocks - 2).wait()
            put(blocks - 1).wait()


def combine_kernel(count, rows, gates, src, out, obuf, sem):
    top = rows.shape[1]
    total = count[0]
    tiles = (total + TC - 1) // TC

    def load(j, s):
        return pltpu.make_async_copy(src.at[pl.ds(pl.multiple_of(j * TC, TC), TC)], obuf.at[s], sem.at[s])

    out[...] = jnp.zeros_like(out)

    @pl.when(tiles > 0)
    def _():
        load(0, 0).start()

    def tile(j, c):
        s = lax.rem(j, 2)

        @pl.when(j + 1 < tiles)
        def _():
            load(j + 1, 1 - s).start()

        col = lax.broadcasted_iota(jnp.int32, (rows.shape[0], TC), 1) + j * TC
        g = jnp.zeros((rows.shape[0], TC), jnp.float32)
        for k in range(top):
            g = g + jnp.where(rows[:, k:k + 1] == col, gates[:, k:k + 1], 0.0)
        g1 = g.astype(jnp.bfloat16)
        rest = g - g1.astype(jnp.float32)
        g2 = rest.astype(jnp.bfloat16)
        g3 = (rest - g2.astype(jnp.float32)).astype(jnp.bfloat16)
        load(j, s).wait()
        row = lax.broadcasted_iota(jnp.int32, (TC, obuf.shape[2]), 0) + j * TC
        o = jnp.where(row < total, obuf[s].astype(jnp.float32), 0.0).astype(jnp.bfloat16)
        out[...] += jnp.dot(jnp.concatenate([g1, g2, g3], axis=1), jnp.concatenate([o, o, o], axis=0),
                            preferred_element_type=jnp.float32)
        return c

    lax.fori_loop(0, tiles, tile, 0)


def solution(mesh):
    tp = mesh.shape['tp']
    ep = mesh.shape['ep']
    tok_spec = P(('dp', 'tp', 'ep'), None)

    def local(x, route_idx, gates, w1, w3, w2):
        t_loc, d = x.shape
        top = route_idx.shape[1]
        e_loc, _, f = w1.shape
        n_tok = t_loc * tp * ep
        n_half = n_tok // 2
        z = lax.axis_index('tp')
        j = lax.axis_index('ep')
        last = (z == tp - 1)
        end = jnp.logical_or(z == 0, last)
        side = jnp.where(z >= tp // 2, 1, 0)

        info = lax.all_gather(jnp.concatenate([route_idx.astype(jnp.float32), gates], axis=1), ('tp', 'ep'), axis=0, tiled=True)
        xa = lax.all_gather(x, ('tp', 'ep'), axis=0, tiled=True)

        loc = info[:, :top].astype(jnp.int32) - j * e_loc
        ga = info[:, top:]
        ids = jnp.arange(e_loc, dtype=jnp.int32)
        hit = jnp.any(loc.T[None] == ids[:, None, None], axis=1)
        before = jnp.arange(n_half)[:, None] < jnp.arange(n_half)[None, :]
        hit2 = hit.reshape(e_loc * 2, n_half)
        pos = jnp.dot(hit2.astype(jnp.bfloat16), before.astype(jnp.bfloat16),
                      preferred_element_type=jnp.float32).astype(jnp.int32).reshape(e_loc, 2, n_half)
        n = jnp.sum(hit2.astype(jnp.int32), axis=1).reshape(e_loc, 2)
        nb = (n + 7) // 8
        off = jnp.sum(jnp.where(ids[:, None, None] > ids[None, :, None], nb[None], 0), axis=1)
        total = jnp.sum(nb, axis=0) * 8
        meta = jnp.stack([nb[:, 0] + nb[:, 1], nb[:, 0], off[:, 0], off[:, 1]], axis=1)
        base = jnp.stack([jnp.zeros_like(nb[:, 0]), nb[:, 0] * 8], axis=1)
        dest = jnp.where(hit, (base[:, :, None] + pos).reshape(e_loc, n_tok), -1)

        full = -(-(n_half * top + 7 * e_loc) // TC) * TC
        part = pl.pallas_call(
            expert_kernel,
            grid_spec=pltpu.PrefetchScalarGridSpec(
                num_scalar_prefetch=1,
                grid=(e_loc,),
                in_specs=[
                    pl.BlockSpec((1, 1, n_tok), lambda e, m: (e, 0, 0)),
                    pl.BlockSpec((n_tok, d), lambda e, m: (0, 0)),
                    pl.BlockSpec((1, d, f), lambda e, m: (e, 0, 0)),
                    pl.BlockSpec((1, d, f), lambda e, m: (e, 0, 0)),
                    pl.BlockSpec((1, f, d), lambda e, m: (e, 0, 0)),
                ],
                out_specs=pl.BlockSpec(memory_space=pl.ANY),
                scratch_shapes=[
                    pltpu.VMEM((2, TM, d), jnp.float32),
                    pltpu.SMEM((3,), jnp.int32),
                    pltpu.SemaphoreType.DMA((2,)),
                ]),
            out_shape=jax.ShapeDtypeStruct((2, full, d), jnp.float32),
            compiler_params=pltpu.CompilerParams(dimension_semantics=('arbitrary',), vmem_limit_bytes=60000 * 1024),
            name='experts',
        )(meta, dest.reshape(e_loc, 1, n_tok), xa, w1, w3, w2)

        def chain(size, ident):
            return pl.pallas_call(
                functools.partial(chain_kernel, tp, size // BR),
                in_specs=[pl.BlockSpec(memory_space=pl.ANY)],
                out_specs=pl.BlockSpec(memory_space=pl.ANY),
                out_shape=jax.ShapeDtypeStruct((full, d), jnp.bfloat16),
                scratch_shapes=[
                    pltpu.VMEM((2, NO, BR, d), jnp.float32),
                    pltpu.VMEM((2, NS, BR, d), jnp.float32),
                    pltpu.VMEM((2, NS, BR, d), jnp.float32),
                    pltpu.VMEM((2, BR, d), jnp.bfloat16),
                    pltpu.SemaphoreType.DMA((2, NO)),
                    pltpu.SemaphoreType.DMA((2, NS)),
                    pltpu.SemaphoreType.DMA((2, NS)),
                    pltpu.SemaphoreType.DMA((2,)),
                    pltpu.SemaphoreType.REGULAR((2,)),
                ],
                compiler_params=pltpu.CompilerParams(collective_id=ident, has_side_effects=True, vmem_limit_bytes=60000 * 1024),
                name=f'chain{size}',
            )

        sizes = tuple(s for s in SIZES if s < full) + (full,)
        need = jnp.max(total)
        which = jnp.sum((need > jnp.array(sizes[:-1], jnp.int32)).astype(jnp.int32))
        o = lax.switch(which, [chain(s, i + 1) for i, s in enumerate(sizes)], part)

        row = (off[:, :, None] * 8 + pos)[:, side]
        mine = loc.reshape(2, n_half, top)[side]
        same = mine[:, :, None] == ids[None, None, :]
        rows = jnp.sum(jnp.where(same, row.T[:, None, :], 0), axis=2)
        rows = jnp.where(jnp.any(same, axis=2), rows, -1)
        order = lambda v: v.reshape(tp // 2, ep, t_loc, top).transpose(1, 0, 2, 3).reshape(n_half, top)
        count = jnp.where(end, total[side], 0).reshape(1)
        py = pl.pallas_call(
            combine_kernel,
            in_specs=[
                pl.BlockSpec(memory_space=pltpu.SMEM),
                pl.BlockSpec(memory_space=pltpu.VMEM),
                pl.BlockSpec(memory_space=pltpu.VMEM),
                pl.BlockSpec(memory_space=pl.ANY),
            ],
            out_specs=pl.BlockSpec(memory_space=pltpu.VMEM),
            out_shape=jax.ShapeDtypeStruct((n_half, d), jnp.float32),
            scratch_shapes=[pltpu.VMEM((2, TC, d), jnp.bfloat16), pltpu.SemaphoreType.DMA((2,))],
            compiler_params=pltpu.CompilerParams(vmem_limit_bytes=60000 * 1024),
            name='combine',
        )(count, order(rows), order(ga.reshape(2, n_half, top)[side]), o)

        y = lax.psum_scatter(py.reshape(ep, n_half // ep, d), 'ep', scatter_dimension=0, tiled=False)
        y = y.astype(jnp.bfloat16).reshape(2, t_loc, d)
        own = jnp.where(last, y[1], y[0])
        got = lax.ppermute(jnp.where(last, y[0], y[1]), 'tp', [(0, 1), (tp - 1, tp - 2)])
        return jnp.where(end, own, got)

    return jax.shard_map(local, mesh=mesh,
                         in_specs=(tok_spec, tok_spec, tok_spec, P('ep', None, 'tp'), P('ep', None, 'tp'), P('ep', 'tp', None)),
                         out_specs=tok_spec, check_vma=False)
```

```python
import functools

import jax
import jax.numpy as jnp
from jax import lax
from jax.experimental import pallas as pl
from jax.experimental.pallas import tpu as pltpu
from jax.sharding import PartitionSpec as P

TM = 128
BR = 16
LAG = 2
NS = 6
NO = NS + 1
TC = 128
SIZES = (640, 768, 896, 1024, 1152, 1280, 1408, 1536, 1792, 2304)
MESH = pl.DeviceIdType.MESH


def expert_kernel(meta, dest, x, w1, w3, w2, out, obuf, cnt, sem):
    e = pl.program_id(0)
    n_tok = x.shape[0]

    def drain(slot):
        def one(_, c):
            pltpu.make_async_copy(obuf.at[slot, pl.ds(0, 8)], out.at[0, pl.ds(0, 8)], sem.at[slot]).wait()
            return c
        lax.fori_loop(0, cnt[slot], one, 0)

    @pl.when(e == 0)
    def _():
        cnt[0] = 0
        cnt[1] = 0
        cnt[2] = 0

    blocks, blocks0, off0, off1 = meta[e, 0], meta[e, 1], meta[e, 2], meta[e, 3]

    def tile(i, c):
        rows = lax.broadcasted_iota(jnp.int32, (TM, n_tok), 0) + i * TM
        pick = jnp.where(dest[0] == rows, 1.0, 0.0).astype(jnp.bfloat16)
        xs = jnp.dot(pick, x[...], preferred_element_type=jnp.float32).astype(jnp.bfloat16)
        a = jnp.dot(xs, w1[0], preferred_element_type=jnp.float32)
        b = jnp.dot(xs, w3[0], preferred_element_type=jnp.float32)
        h = (jax.nn.silu(a) * b).astype(jnp.bfloat16)
        slot = cnt[2]
        drain(slot)
        obuf[slot] = jnp.dot(h, w2[0], preferred_element_type=jnp.float32)
        first = i * (TM // 8)
        n = jnp.minimum(TM // 8, blocks - first)

        def put(k, c):
            g = first + k
            late = g >= blocks0
            half = jnp.where(late, 1, 0)
            to = jnp.where(late, off1 + g - blocks0, off0 + g)
            pltpu.make_async_copy(
                obuf.at[slot, pl.ds(pl.multiple_of(k * 8, 8), 8)],
                out.at[half, pl.ds(pl.multiple_of(to * 8, 8), 8)], sem.at[slot]).start()
            return c

        lax.fori_loop(0, n, put, 0)
        cnt[slot] = n
        cnt[2] = 1 - slot
        return c

    lax.fori_loop(0, (blocks + TM // 8 - 1) // (TM // 8), tile, 0)

    @pl.when(e == pl.num_programs(0) - 1)
    def _():
        drain(0)
        drain(1)


def chain_kernel(n, blocks, count, rows, gates, src, out, own, rbuf, sbuf, obuf, own_sem, send_sem, recv_sem, credit):
    z = lax.axis_index('tp')
    barrier = pltpu.get_barrier_semaphore()

    @pl.when(z > 0)
    def _():
        pl.semaphore_signal(barrier, inc=1, device_id={'tp': z - 1}, device_id_type=MESH)

    @pl.when(z < n - 1)
    def _():
        pl.semaphore_signal(barrier, inc=1, device_id={'tp': z + 1}, device_id_type=MESH)

    pl.semaphore_wait(barrier, jnp.where(z > 0, 1, 0) + jnp.where(z < n - 1, 1, 0))

    def load(d, k):
        s = lax.rem(k, NO)
        return pltpu.make_async_copy(src.at[1 - d, pl.ds(pl.multiple_of(k * BR, BR), BR)], own.at[d, s], own_sem.at[d, s])

    def send(d, k, buf, s_buf):
        s = lax.rem(k, NS)
        to = z + 1 if d == 0 else z - 1
        return pltpu.make_async_remote_copy(
            src_ref=buf.at[d, s_buf], dst_ref=rbuf.at[d, s], send_sem=send_sem.at[d, s], recv_sem=recv_sem.at[d, s],
            device_id={'tp': to}, device_id_type=MESH)

    per = TC // BR

    def gated(j):
        col = lax.broadcasted_iota(jnp.int32, (rows.shape[0], TC), 1) + j * TC
        g = jnp.zeros((rows.shape[0], TC), jnp.float32)
        for k in range(rows.shape[1]):
            g = g + jnp.where(rows[:, k:k + 1] == col, gates[:, k:k + 1], 0.0)
        g1 = g.astype(jnp.bfloat16)
        rest = g - g1.astype(jnp.float32)
        g2 = rest.astype(jnp.bfloat16)
        g3 = (rest - g2.astype(jnp.float32)).astype(jnp.bfloat16)
        g = jnp.concatenate([g1, g2, g3], axis=1)
        wide = min(512, out.shape[1])
        row = lax.broadcasted_iota(jnp.int32, (TC, wide), 0) + j * TC

        def columns(q, c):
            at = pl.ds(pl.multiple_of(q * wide, wide), wide)
            o = jnp.where(row < count[0], obuf[:, at].astype(jnp.float32), 0.0).astype(jnp.bfloat16)
            out[:, at] += jnp.dot(g, jnp.concatenate([o, o, o], axis=0), preferred_element_type=jnp.float32)
            return c

        lax.fori_loop(0, out.shape[1] // wide, columns, 0)

    def step(i, c):
        work = []
        for d in (0, 1):
            p = z if d == 0 else n - 1 - z
            k = i - LAG * p
            work.append((d, p, k, jnp.logical_and(k >= 0, k < blocks)))

        for d, p, k, live in work:
            @pl.when(live)
            def _(d=d, p=p, k=k):
                @pl.when(jnp.logical_and(p < n - 1, k >= NS))
                def _():
                    send(d, k - NS, sbuf, lax.rem(k, NS)).wait_send()

                @pl.when(k == 0)
                def _():
                    load(d, k).start()

                @pl.when(k + 1 < blocks)
                def _():
                    load(d, k + 1).start()

                load(d, k).wait()

        for d, p, k, live in work:
            @pl.when(jnp.logical_and(live, p == 0))
            def _(d=d, k=k):
                @pl.when(k >= NS)
                def _():
                    pl.semaphore_wait(credit.at[d], 1)
                send(d, k, own, lax.rem(k, NO)).start()

        for d, p, k, live in work:
            @pl.when(jnp.logical_and(live, p > 0))
            def _(d=d, p=p, k=k):
                s = lax.rem(k, NS)
                send(d, k, sbuf, s).wait_recv()

                @pl.when(p < n - 1)
                def _():
                    sbuf[d, s] = rbuf[d, s] + own[d, lax.rem(k, NO)]

                @pl.when(p == n - 1)
                def _():
                    to = pl.multiple_of(lax.rem(k, per) * BR, BR)
                    obuf[pl.ds(to, BR)] = (rbuf[d, s] + own[d, lax.rem(k, NO)]).astype(jnp.bfloat16)

                @pl.when(k + NS < blocks)
                def _():
                    back = z - 1 if d == 0 else z + 1
                    pl.semaphore_signal(credit.at[d], inc=1, device_id={'tp': back}, device_id_type=MESH)

        for d, p, k, live in work:
            @pl.when(jnp.logical_and(live, jnp.logical_and(p > 0, p < n - 1)))
            def _(d=d, k=k):
                @pl.when(k >= NS)
                def _():
                    pl.semaphore_wait(credit.at[d], 1)
                send(d, k, sbuf, lax.rem(k, NS)).start()

        k = i - LAG * (n - 1)

        @pl.when(jnp.logical_and(jnp.logical_or(z == 0, z == n - 1), jnp.logical_and(k >= 0, lax.rem(k + per, per) == per - 1)))
        def _():
            gated(k // per)
        return c

    @pl.when(jnp.logical_or(z == 0, z == n - 1))
    def _():
        out[...] = jnp.zeros_like(out)

    lax.fori_loop(0, blocks + LAG * (n - 1), step, 0)

    for d in (0, 1):
        p = z if d == 0 else n - 1 - z

        @pl.when(p < n - 1)
        def _(d=d):
            for k in range(blocks - NS, blocks):
                send(d, k, sbuf, k % NS).wait_send()


def gather_kernel(n, x, info, xout, iout, xbuf, ibuf, own_sem, xsend, isend, xrecv, irecv, out_sem):
    z = lax.axis_index('tp')
    j = lax.axis_index('ep')
    t_loc = x.shape[0]
    sib = j + 1 - 2 * lax.rem(j, 2)
    peer = lax.rem(j + 2, 4)
    blk = lambda zz, jj: zz * 4 + jj
    up, down = {'tp': z + 1}, {'tp': z - 1}
    me = blk(z, j)
    mine = (pltpu.make_async_copy(x, xbuf.at[me], own_sem.at[0]), pltpu.make_async_copy(info, ibuf.at[me], own_sem.at[1]))
    for m in mine:
        m.start()

    barrier = pltpu.get_barrier_semaphore()
    for other in (sib, peer):
        pl.semaphore_signal(barrier, inc=1, device_id={'ep': other}, device_id_type=MESH)

    @pl.when(z > 0)
    def _():
        pl.semaphore_signal(barrier, inc=1, device_id=down, device_id_type=MESH)

    @pl.when(z < n - 1)
    def _():
        pl.semaphore_signal(barrier, inc=1, device_id=up, device_id_type=MESH)

    pl.semaphore_wait(barrier, 2 + jnp.where(z > 0, 1, 0) + jnp.where(z < n - 1, 1, 0))

    def copies(b, i, dev):
        make = lambda buf, s, r: pltpu.make_async_remote_copy(
            src_ref=buf.at[b], dst_ref=buf.at[b], send_sem=s.at[i], recv_sem=r.at[b], device_id=dev, device_id_type=MESH)
        return make(ibuf, isend, irecv), make(xbuf, xsend, xrecv)

    def send(b, i, dev):
        for c in copies(b, i, dev):
            c.start()

    def sent(b, i, dev):
        for c in copies(b, i, dev):
            c.wait_send()

    def arrive(b):
        for c in copies(b, 0, {'ep': sib}):
            c.wait_recv()

    def keep(b):
        return pltpu.make_async_copy(xbuf.at[b], xout.at[pl.ds(pl.multiple_of(b * t_loc, t_loc), t_loc)], out_sem.at[b])

    def line(f):
        f(z, 0, True, True)
        for r in range(1, n):
            @pl.when(z >= r)
            def _(r=r):
                f(z - r, r, True, False)

            @pl.when(z + r < n)
            def _(r=r):
                f(z + r, r, False, True)

    def spread(act):
        def f(zz, r, ups, downs):
            b = blk(zz, j)
            if act is send:
                if r == 0:
                    for m in mine:
                        m.wait()
                else:
                    arrive(b)
            if ups:
                @pl.when(z < n - 1)
                def _():
                    act(b, r, up)
            if downs:
                @pl.when(z > 0)
                def _():
                    act(b, n + r, down)
            act(b, 2 * n + zz, {'ep': peer})
            act(b, 3 * n + zz, {'ep': sib})
            if act is send:
                keep(b).start()
        return f

    def relay(act):
        def f(zz, r, ups, downs):
            b = blk(zz, peer)
            if act is send:
                arrive(b)
            act(b, 4 * n + zz, {'ep': sib})
            if act is send:
                keep(b).start()
        return f

    line(spread(send))
    line(relay(send))
    for other in (sib, lax.rem(sib + 2, 4)):
        def take(zz, r, ups, downs, other=other):
            arrive(blk(zz, other))
            keep(blk(zz, other)).start()
        line(take)
    every = pltpu.make_async_copy(ibuf, iout, own_sem.at[0])
    every.start()
    line(spread(sent))
    line(relay(sent))
    for b in range(4 * n):
        keep(b).wait()
    every.wait()


def finish_kernel(n, py, out, ra, sb, rb, yb, rc, a_send, a_recv, b_send, b_recv, c_send, c_recv):
    z = lax.axis_index('tp')
    j = lax.axis_index('ep')
    t_loc = out.shape[0]
    ln = t_loc // 2
    y, c = j // 2, lax.rem(j, 2)
    sib = j + 1 - 2 * c
    peer = lax.rem(j + 2, 4)
    end = jnp.logical_or(z == 0, z == n - 1)
    low = z < n // 2
    across = jnp.where(z == 0, 1, jnp.where(z == 1, 0, jnp.where(z == n - 1, n - 2, n - 1)))
    barrier = pltpu.get_barrier_semaphore()
    pl.semaphore_signal(barrier, inc=1, device_id={'tp': across}, device_id_type=MESH)

    @pl.when(end)
    def _():
        for other in (sib, peer):
            pl.semaphore_signal(barrier, inc=1, device_id={'ep': other}, device_id_type=MESH)

    pl.semaphore_wait(barrier, jnp.where(end, 3, 1))

    inner = jnp.where(low, 1, 0)
    starts = [pl.multiple_of((inner if q < 2 else 1 - inner) * t_loc + (q % 2) * ln, ln) for q in range(4)]

    def to_sib(q, yy):
        at = pl.ds(starts[q], ln)
        return pltpu.make_async_remote_copy(
            src_ref=py.at[2 * yy + 1 - c, at], dst_ref=ra.at[yy, at], send_sem=a_send.at[q, yy], recv_sem=a_recv.at[q, yy],
            device_id={'ep': sib}, device_id_type=MESH)

    def to_peer(q):
        at = pl.ds(starts[q], ln)
        return pltpu.make_async_remote_copy(
            src_ref=sb.at[at], dst_ref=rb.at[at], send_sem=b_send.at[q], recv_sem=b_recv.at[q],
            device_id={'ep': peer}, device_id_type=MESH)

    def to_inner(q):
        return pltpu.make_async_remote_copy(
            src_ref=yb.at[q], dst_ref=rc.at[q], send_sem=c_send.at[q], recv_sem=c_recv.at[q],
            device_id={'tp': across}, device_id_type=MESH)

    @pl.when(end)
    def _():
        for q in range(4):
            to_sib(q, 1 - y).start()
        for q in range(4):
            to_sib(q, y).start()
        for q in range(4):
            at = pl.ds(starts[q], ln)
            to_sib(q, 1 - y).wait_recv()
            sb[at] = py[2 * (1 - y) + c, at] + ra[1 - y, at]
            to_peer(q).start()
        for q in range(4):
            at = pl.ds(starts[q], ln)
            to_sib(q, y).wait_recv()
            to_peer(q).wait_recv()
            v = ((py[2 * y + c, at] + ra[y, at]) + rb[at]).astype(jnp.bfloat16)
            if q < 2:
                yb[q] = v
                to_inner(q).start()
            else:
                out[pl.ds((q - 2) * ln, ln)] = v
        for q in range(4):
            to_sib(q, y).wait_send()
            to_sib(q, 1 - y).wait_send()
            to_peer(q).wait_send()
        for q in range(2):
            to_inner(q).wait_send()

    @pl.when(jnp.logical_not(end))
    def _():
        for q in range(2):
            to_inner(q).wait_recv()
            out[pl.ds(q * ln, ln)] = rc[q]


def solution(mesh):
    tp = mesh.shape['tp']
    ep = mesh.shape['ep']
    tok_spec = P(('dp', 'tp', 'ep'), None)

    def local(x, route_idx, gates, w1, w3, w2):
        t_loc, d = x.shape
        top = route_idx.shape[1]
        e_loc, _, f = w1.shape
        n_tok = t_loc * tp * ep
        n_half = n_tok // 2
        z = lax.axis_index('tp')
        j = lax.axis_index('ep')
        side = jnp.where(z >= tp // 2, 1, 0)

        own = jnp.concatenate([route_idx.astype(jnp.float32), gates], axis=1)
        ir = t_loc * 2 * top // 128
        any_ = pl.BlockSpec(memory_space=pl.ANY)
        vmem = pl.BlockSpec(memory_space=pltpu.VMEM)
        xa, info = pl.pallas_call(
            functools.partial(gather_kernel, tp),
            in_specs=[any_, any_],
            out_specs=[any_, any_],
            out_shape=[jax.ShapeDtypeStruct((n_tok, d), x.dtype), jax.ShapeDtypeStruct((tp * ep, ir, 128), jnp.float32)],
            scratch_shapes=[
                pltpu.VMEM((tp * ep, t_loc, d), x.dtype),
                pltpu.VMEM((tp * ep, ir, 128), jnp.float32),
                pltpu.SemaphoreType.DMA((2,)),
                pltpu.SemaphoreType.DMA((5 * tp,)),
                pltpu.SemaphoreType.DMA((5 * tp,)),
                pltpu.SemaphoreType.DMA((tp * ep,)),
                pltpu.SemaphoreType.DMA((tp * ep,)),
                pltpu.SemaphoreType.DMA((tp * ep,)),
            ],
            compiler_params=pltpu.CompilerParams(collective_id=20, has_side_effects=True),
            name='gather',
        )(x, own.reshape(ir, 128))
        info = info.reshape(n_tok, 2 * top)

        loc = info[:, :top].astype(jnp.int32) - j * e_loc
        ga = info[:, top:]
        ids = jnp.arange(e_loc, dtype=jnp.int32)
        hit = jnp.any(loc.T[None] == ids[:, None, None], axis=1)
        before = jnp.arange(n_half)[:, None] < jnp.arange(n_half)[None, :]
        hit2 = hit.reshape(e_loc * 2, n_half)
        pos = jnp.dot(hit2.astype(jnp.bfloat16), before.astype(jnp.bfloat16),
                      preferred_element_type=jnp.float32).astype(jnp.int32).reshape(e_loc, 2, n_half)
        n = jnp.sum(hit2.astype(jnp.int32), axis=1).reshape(e_loc, 2)
        nb = (n + 7) // 8
        off = jnp.sum(jnp.where(ids[:, None, None] > ids[None, :, None], nb[None], 0), axis=1)
        total = jnp.sum(nb, axis=0) * 8
        meta = jnp.stack([nb[:, 0] + nb[:, 1], nb[:, 0], off[:, 0], off[:, 1]], axis=1)
        base = jnp.stack([jnp.zeros_like(nb[:, 0]), nb[:, 0] * 8], axis=1)
        dest = jnp.where(hit, (base[:, :, None] + pos).reshape(e_loc, n_tok), -1)

        full = -(-(n_half * top + 7 * e_loc) // TC) * TC
        part = pl.pallas_call(
            expert_kernel,
            grid_spec=pltpu.PrefetchScalarGridSpec(
                num_scalar_prefetch=1,
                grid=(e_loc,),
                in_specs=[
                    pl.BlockSpec((1, 1, n_tok), lambda e, m: (e, 0, 0)),
                    pl.BlockSpec((n_tok, d), lambda e, m: (0, 0)),
                    pl.BlockSpec((1, d, f), lambda e, m: (e, 0, 0)),
                    pl.BlockSpec((1, d, f), lambda e, m: (e, 0, 0)),
                    pl.BlockSpec((1, f, d), lambda e, m: (e, 0, 0)),
                ],
                out_specs=pl.BlockSpec(memory_space=pl.ANY),
                scratch_shapes=[
                    pltpu.VMEM((2, TM, d), jnp.float32),
                    pltpu.SMEM((3,), jnp.int32),
                    pltpu.SemaphoreType.DMA((2,)),
                ]),
            out_shape=jax.ShapeDtypeStruct((2, full, d), jnp.float32),
            compiler_params=pltpu.CompilerParams(dimension_semantics=('arbitrary',), vmem_limit_bytes=60000 * 1024),
            name='experts',
        )(meta, dest.reshape(e_loc, 1, n_tok), xa, w1, w3, w2)

        row = (off[:, :, None] * 8 + pos)[:, side]
        mine = loc.reshape(2, n_half, top)[side]
        same = mine[:, :, None] == ids[None, None, :]
        rows = jnp.sum(jnp.where(same, row.T[:, None, :], 0), axis=2)
        rows = jnp.where(jnp.any(same, axis=2), rows, -1)
        order = lambda v: v.reshape(tp // 2, ep, t_loc, top).transpose(1, 0, 2, 3).reshape(n_half, top)

        def chain(size, ident):
            return pl.pallas_call(
                functools.partial(chain_kernel, tp, size // BR),
                in_specs=[pl.BlockSpec(memory_space=pltpu.SMEM), vmem, vmem, any_],
                out_specs=vmem,
                out_shape=jax.ShapeDtypeStruct((n_half, d), jnp.float32),
                scratch_shapes=[
                    pltpu.VMEM((2, NO, BR, d), jnp.float32),
                    pltpu.VMEM((2, NS, BR, d), jnp.float32),
                    pltpu.VMEM((2, NS, BR, d), jnp.float32),
                    pltpu.VMEM((TC, d), jnp.bfloat16),
                    pltpu.SemaphoreType.DMA((2, NO)),
                    pltpu.SemaphoreType.DMA((2, NS)),
                    pltpu.SemaphoreType.DMA((2, NS)),
                    pltpu.SemaphoreType.REGULAR((2,)),
                ],
                compiler_params=pltpu.CompilerParams(collective_id=ident, has_side_effects=True, vmem_limit_bytes=60000 * 1024),
                name=f'chain{size}',
            )

        sizes = tuple(s for s in SIZES if s < full) + (full,)
        need = jnp.max(total)
        which = jnp.sum((need > jnp.array(sizes[:-1], jnp.int32)).astype(jnp.int32))
        py = lax.switch(which, [chain(s, i + 1) for i, s in enumerate(sizes)],
                        total[side].reshape(1), order(rows), order(ga.reshape(2, n_half, top)[side]), part)

        return pl.pallas_call(
            functools.partial(finish_kernel, tp),
            in_specs=[vmem],
            out_specs=vmem,
            out_shape=jax.ShapeDtypeStruct((t_loc, d), x.dtype),
            scratch_shapes=[
                pltpu.VMEM((2, 2 * t_loc, d), jnp.float32),
                pltpu.VMEM((2 * t_loc, d), jnp.float32),
                pltpu.VMEM((2 * t_loc, d), jnp.float32),
                pltpu.VMEM((2, t_loc // 2, d), x.dtype),
                pltpu.VMEM((2, t_loc // 2, d), x.dtype),
                pltpu.SemaphoreType.DMA((4, 2)),
                pltpu.SemaphoreType.DMA((4, 2)),
                pltpu.SemaphoreType.DMA((4,)),
                pltpu.SemaphoreType.DMA((4,)),
                pltpu.SemaphoreType.DMA((2,)),
                pltpu.SemaphoreType.DMA((2,)),
            ],
            compiler_params=pltpu.CompilerParams(collective_id=21, has_side_effects=True, vmem_limit_bytes=60000 * 1024),
            name='finish',
        )(py.reshape(ep, n_half // ep, d))

    return jax.shard_map(local, mesh=mesh,
                         in_specs=(tok_spec, tok_spec, tok_spec, P('ep', None, 'tp'), P('ep', None, 'tp'), P('ep', 'tp', None)),
                         out_specs=tok_spec, check_vma=False)
```

```python
import functools

import jax
import jax.numpy as jnp
from jax import lax
from jax.experimental import pallas as pl
from jax.experimental.pallas import tpu as pltpu
from jax.sharding import PartitionSpec as P

BR = 16
LAG = 2
NS = 6
TC = 128
SIZES = (768, 896, 1024, 1152, 1280, 1408, 1536, 2048)
MESH = pl.DeviceIdType.MESH


def chain_kernel(n, blocks, count, rows, gates, dest, hid, w2, out, hbuf, wbuf, pick, own, rbuf, sbuf, obuf,
                 h_sem, w_sem, send_sem, recv_sem, credit):
    z = lax.axis_index('tp')
    n_exp, f, d_out = wbuf.shape
    n_half = dest.shape[3]
    tiles = blocks * BR // TC

    def h_load(e):
        at = pl.ds(pl.multiple_of(e * f, f), f)
        return pltpu.make_async_copy(hid.at[:, at], hbuf.at[:, at], h_sem.at[e])

    def w_load(e):
        return pltpu.make_async_copy(w2.at[e], wbuf.at[e], w_sem.at[e])

    for e in range(n_exp):
        h_load(e).start()
    for e in range(n_exp):
        w_load(e).start()

    barrier = pltpu.get_barrier_semaphore()

    @pl.when(z > 0)
    def _():
        pl.semaphore_signal(barrier, inc=1, device_id={'tp': z - 1}, device_id_type=MESH)

    @pl.when(z < n - 1)
    def _():
        pl.semaphore_signal(barrier, inc=1, device_id={'tp': z + 1}, device_id_type=MESH)

    def gather(half, t, e):
        row = lax.broadcasted_iota(jnp.int32, (TC, n_half), 0) + t * TC
        one = jnp.where(dest[half, e] == row, 1.0, 0.0).astype(jnp.bfloat16)
        at = pl.ds(pl.multiple_of(e * f, f), f)
        got = jnp.dot(one, hbuf[pl.ds(pl.multiple_of(half * n_half, n_half), n_half), at], preferred_element_type=jnp.float32)
        return got.astype(jnp.bfloat16), at

    def first(e, c):
        h_load(e).wait()

        def one(q, c):
            got, at = gather(q // 2, q % 2, e)
            pick[q // 2, q % 2, :, at] = got
            return c
        return lax.fori_loop(0, 2 * min(2, tiles), one, c) if tiles > 1 else lax.fori_loop(0, 2, lambda h, c: one(2 * h, c), c)

    lax.fori_loop(0, n_exp, first, 0)
    own[:, 0] = jnp.zeros_like(own[:, 0])

    def second(e, c):
        w_load(e).wait()

        def one(half, c):
            at = pl.ds(pl.multiple_of(e * f, f), f)
            own[half, 0] += jnp.dot(pick[half, 0, :, at], wbuf[e], preferred_element_type=jnp.float32)
            return c
        return lax.fori_loop(0, 2, one, c)

    lax.fori_loop(0, n_exp, second, 0)

    pl.semaphore_wait(barrier, jnp.where(z > 0, 1, 0) + jnp.where(z < n - 1, 1, 0))

    def mine(d, k):
        return own.at[1 - d, lax.rem(k // (TC // BR), 3), pl.ds(pl.multiple_of(lax.rem(k, TC // BR) * BR, BR), BR)]

    def send(d, k, buf):
        s = lax.rem(k, NS)
        to = z + 1 if d == 0 else z - 1
        return pltpu.make_async_remote_copy(
            src_ref=buf, dst_ref=rbuf.at[d, s], send_sem=send_sem.at[d, s], recv_sem=recv_sem.at[d, s],
            device_id={'tp': to}, device_id_type=MESH)

    def passed(d, k):
        return sbuf.at[d, lax.rem(k, NS)]

    per = TC // BR

    def gated(j):
        col = lax.broadcasted_iota(jnp.int32, (rows.shape[0], TC), 1) + j * TC
        g = jnp.zeros((rows.shape[0], TC), jnp.float32)
        for k in range(rows.shape[1]):
            g = g + jnp.where(rows[:, k:k + 1] == col, gates[:, k:k + 1], 0.0)
        g1 = g.astype(jnp.bfloat16)
        rest = g - g1.astype(jnp.float32)
        g2 = rest.astype(jnp.bfloat16)
        g3 = (rest - g2.astype(jnp.float32)).astype(jnp.bfloat16)
        g = jnp.concatenate([g1, g2, g3], axis=1)
        wide = min(256, out.shape[1])
        row = lax.broadcasted_iota(jnp.int32, (TC, wide), 0) + j * TC

        def columns(q, c):
            at = pl.ds(pl.multiple_of(q * wide, wide), wide)
            o = jnp.where(row < count[0], obuf[:, at].astype(jnp.float32), 0.0).astype(jnp.bfloat16)
            out[:, at] += jnp.dot(g, jnp.concatenate([o, o, o], axis=0), preferred_element_type=jnp.float32)
            return c

        lax.fori_loop(0, out.shape[1] // wide, columns, 0)

    wide_own = d_out // per

    def step(i, c):
        tile, part = i // per, lax.rem(i, per)

        @pl.when(tile + 1 < tiles)
        def _():
            def one(half, c):
                at = pl.ds(pl.multiple_of(part * wide_own, wide_own), wide_own)
                own[half, lax.rem(tile + 1, 3), :, at] = jnp.dot(
                    pick[half, lax.rem(tile + 1, 2)], wbuf[:, :, at].reshape(n_exp * f, wide_own),
                    preferred_element_type=jnp.float32)
                return c
            lax.fori_loop(0, 2, one, 0)

        work = []
        for d in (0, 1):
            p = z if d == 0 else n - 1 - z
            k = i - LAG * p
            work.append((d, p, k, jnp.logical_and(k >= 0, k < blocks)))

        for d, p, k, live in work:
            @pl.when(jnp.logical_and(live, jnp.logical_and(p < n - 1, k >= NS)))
            def _(d=d, k=k):
                send(d, k - NS, passed(d, k)).wait_send()

            @pl.when(jnp.logical_and(live, p == 0))
            def _(d=d, k=k):
                @pl.when(k >= NS)
                def _():
                    pl.semaphore_wait(credit.at[d], 1)
                send(d, k, mine(d, k)).start()

        for d, p, k, live in work:
            @pl.when(jnp.logical_and(live, p > 0))
            def _(d=d, p=p, k=k):
                s = lax.rem(k, NS)
                send(d, k, passed(d, k)).wait_recv()

                @pl.when(p < n - 1)
                def _():
                    sbuf[d, s] = rbuf[d, s] + mine(d, k)[...]

                @pl.when(p == n - 1)
                def _():
                    to = pl.multiple_of(lax.rem(k, per) * BR, BR)
                    obuf[pl.ds(to, BR)] = (rbuf[d, s] + mine(d, k)[...]).astype(jnp.bfloat16)

                @pl.when(k + NS < blocks)
                def _():
                    back = z - 1 if d == 0 else z + 1
                    pl.semaphore_signal(credit.at[d], inc=1, device_id={'tp': back}, device_id_type=MESH)

        for d, p, k, live in work:
            @pl.when(jnp.logical_and(live, jnp.logical_and(p > 0, p < n - 1)))
            def _(d=d, k=k):
                @pl.when(k >= NS)
                def _():
                    pl.semaphore_wait(credit.at[d], 1)
                send(d, k, passed(d, k)).start()

        @pl.when(tile + 2 < tiles)
        def _():
            def one(q, c):
                e = part * (n_exp // per) + q // 2
                got, at = gather(q % 2, tile + 2, e)
                pick[q % 2, lax.rem(tile, 2), :, at] = got
                return c
            lax.fori_loop(0, 2 * (n_exp // per), one, 0)

        k = i - LAG * (n - 1)

        @pl.when(jnp.logical_and(jnp.logical_or(z == 0, z == n - 1), jnp.logical_and(k >= 0, lax.rem(k + per, per) == per - 1)))
        def _():
            gated(k // per)
        return c

    @pl.when(jnp.logical_or(z == 0, z == n - 1))
    def _():
        out[...] = jnp.zeros_like(out)

    lax.fori_loop(0, blocks + LAG * (n - 1), step, 0)

    for d in (0, 1):
        p = z if d == 0 else n - 1 - z

        @pl.when(p < n - 1)
        def _(d=d):
            for k in range(blocks - NS, blocks):
                send(d, k, passed(d, k)).wait_send()


def hidden_kernel(n, x, route, gate, w1, w3, hid, rout, gout, xbuf, rbuf, gbuf, w1b, w3b, hbuf,
                  own_sem, w_sem, h_sem, sends, recvs):
    z = lax.axis_index('tp')
    j = lax.axis_index('ep')
    t_loc, d = x.shape
    n_exp, _, f = w1b.shape
    sib = j + 1 - 2 * lax.rem(j, 2)
    peer = lax.rem(j + 2, 4)
    blk = lambda zz, jj: zz * 4 + jj
    up, down = {'tp': z + 1}, {'tp': z - 1}
    me = blk(z, j)
    bufs = (rbuf, gbuf, xbuf)
    mine = [pltpu.make_async_copy(a, b.at[me], own_sem.at[i]) for i, (a, b) in enumerate(zip((route, gate, x), bufs))]
    for m in mine:
        m.start()

    def w_loads(e):
        return (pltpu.make_async_copy(w1.at[e], w1b.at[e], w_sem.at[0, e]),
                pltpu.make_async_copy(w3.at[e], w3b.at[e], w_sem.at[1, e]))

    for e in range(n_exp):
        for c in w_loads(e):
            c.start()

    barrier = pltpu.get_barrier_semaphore()
    for other in (sib, peer):
        pl.semaphore_signal(barrier, inc=1, device_id={'ep': other}, device_id_type=MESH)

    @pl.when(z > 0)
    def _():
        pl.semaphore_signal(barrier, inc=1, device_id=down, device_id_type=MESH)

    @pl.when(z < n - 1)
    def _():
        pl.semaphore_signal(barrier, inc=1, device_id=up, device_id_type=MESH)

    pl.semaphore_wait(barrier, 2 + jnp.where(z > 0, 1, 0) + jnp.where(z < n - 1, 1, 0))

    def copies(b, i, dev):
        return [pltpu.make_async_remote_copy(
            src_ref=buf.at[b], dst_ref=buf.at[b], send_sem=sends.at[a, i], recv_sem=recvs.at[a, b],
            device_id=dev, device_id_type=MESH) for a, buf in enumerate(bufs)]

    def send(b, i, dev):
        for c in copies(b, i, dev):
            c.start()

    def sent(b, i, dev):
        for c in copies(b, i, dev):
            c.wait_send()

    def arrive(b):
        for c in copies(b, 0, {'ep': sib}):
            c.wait_recv()

    first, last = z == 0, z == n - 1
    planes = (z, jnp.where(first, 1, z - 1), jnp.where(first, 2, jnp.where(last, 1, z + 1)), jnp.where(z <= 1, n - 1, 0))

    def line(i, act):
        zz = planes[i]
        b = blk(zz, j)
        if act is send:
            if i == 0:
                for m in mine:
                    m.wait()
            else:
                arrive(b)

        @pl.when(jnp.logical_and(zz <= z, z < n - 1))
        def _():
            act(b, i, up)

        @pl.when(jnp.logical_and(zz >= z, z > 0))
        def _():
            act(b, n + i, down)
        act(b, 2 * n + i, {'ep': peer})
        act(b, 3 * n + i, {'ep': sib})

    def relay(i, act):
        b = blk(planes[i], peer)
        if act is send:
            arrive(b)
        act(b, 4 * n + i, {'ep': sib})

    def full(i):
        arrive(blk(planes[i], sib))
        arrive(blk(planes[i], lax.rem(sib + 2, 4)))

    def put(i):
        at = pl.ds(pl.multiple_of(planes[i] * 4 * t_loc, 4 * t_loc), 4 * t_loc)
        return pltpu.make_async_copy(hbuf.at[i % 2], hid.at[at], h_sem.at[i % 2])

    def compute(i, lo, hi):
        at = pl.ds(planes[i] * 4, 4)

        def one(e, c):
            if i == 0:
                for w in w_loads(e):
                    w.wait()
            rows = xbuf[at].reshape(4 * t_loc, d)
            a = jnp.dot(rows, w1b[e], preferred_element_type=jnp.float32)
            b = jnp.dot(rows, w3b[e], preferred_element_type=jnp.float32)
            named = rbuf[at].reshape(4 * t_loc, 128).astype(jnp.float32) == (j * n_exp + e).astype(jnp.float32)
            hit = jnp.max(jnp.where(named, 1.0, 0.0), axis=1, keepdims=True)
            h = jnp.where(hit > 0.0, jax.nn.silu(a) * b, 0.0)
            hbuf[i % 2, :, pl.ds(pl.multiple_of(e * f, f), f)] = h.astype(jnp.bfloat16)
            return c
        lax.fori_loop(lo, hi, one, 0)

    half = n_exp // 2
    inside = jnp.logical_not(jnp.logical_or(first, last))
    line(0, send)
    relay(0, send)
    line(1, send)

    @pl.when(inside)
    def _():
        line(2, send)
    full(0)
    compute(0, 0, half)

    @pl.when(jnp.logical_not(inside))
    def _():
        line(2, send)
    relay(1, send)
    compute(0, half, n_exp)
    put(0).start()
    line(3, send)
    relay(2, send)
    full(1)
    compute(1, 0, half)
    relay(3, send)
    compute(1, half, n_exp)
    put(1).start()
    full(2)
    put(0).wait()
    compute(2, 0, n_exp)
    put(2).start()
    full(3)
    put(1).wait()
    every = (pltpu.make_async_copy(rbuf, rout, own_sem.at[0]), pltpu.make_async_copy(gbuf, gout, own_sem.at[1]))
    for m in every:
        m.start()
    compute(3, 0, n_exp)
    put(3).start()
    for i in range(n):
        line(i, sent)
        relay(i, sent)
    for m in every:
        m.wait()
    put(2).wait()
    put(3).wait()


def finish_kernel(n, py, out, ra, sb, rb, yb, rc, a_send, a_recv, b_send, b_recv, c_send, c_recv):
    z = lax.axis_index('tp')
    j = lax.axis_index('ep')
    t_loc = out.shape[0]
    ln = t_loc // 2
    y, c = j // 2, lax.rem(j, 2)
    sib = j + 1 - 2 * c
    peer = lax.rem(j + 2, 4)
    end = jnp.logical_or(z == 0, z == n - 1)
    low = z < n // 2
    across = jnp.where(z == 0, 1, jnp.where(z == 1, 0, jnp.where(z == n - 1, n - 2, n - 1)))
    barrier = pltpu.get_barrier_semaphore()
    pl.semaphore_signal(barrier, inc=1, device_id={'tp': across}, device_id_type=MESH)

    @pl.when(end)
    def _():
        for other in (sib, peer):
            pl.semaphore_signal(barrier, inc=1, device_id={'ep': other}, device_id_type=MESH)

    pl.semaphore_wait(barrier, jnp.where(end, 3, 1))

    inner = jnp.where(low, 1, 0)
    starts = [pl.multiple_of((inner if q < 2 else 1 - inner) * t_loc + (q % 2) * ln, ln) for q in range(4)]

    def to_sib(q, yy):
        at = pl.ds(starts[q], ln)
        return pltpu.make_async_remote_copy(
            src_ref=py.at[2 * yy + 1 - c, at], dst_ref=ra.at[yy, at], send_sem=a_send.at[q, yy], recv_sem=a_recv.at[q, yy],
            device_id={'ep': sib}, device_id_type=MESH)

    def to_peer(q):
        at = pl.ds(starts[q], ln)
        return pltpu.make_async_remote_copy(
            src_ref=sb.at[at], dst_ref=rb.at[at], send_sem=b_send.at[q], recv_sem=b_recv.at[q],
            device_id={'ep': peer}, device_id_type=MESH)

    def to_inner(q):
        return pltpu.make_async_remote_copy(
            src_ref=yb.at[q], dst_ref=rc.at[q], send_sem=c_send.at[q], recv_sem=c_recv.at[q],
            device_id={'tp': across}, device_id_type=MESH)

    @pl.when(end)
    def _():
        for q in range(4):
            to_sib(q, 1 - y).start()
        for q in range(4):
            to_sib(q, y).start()
        for q in range(4):
            at = pl.ds(starts[q], ln)
            to_sib(q, 1 - y).wait_recv()
            sb[at] = py[2 * (1 - y) + c, at] + ra[1 - y, at]
            to_peer(q).start()
        for q in range(4):
            at = pl.ds(starts[q], ln)
            to_sib(q, y).wait_recv()
            to_peer(q).wait_recv()
            v = ((py[2 * y + c, at] + ra[y, at]) + rb[at]).astype(jnp.bfloat16)
            if q < 2:
                yb[q] = v
                to_inner(q).start()
            else:
                out[pl.ds((q - 2) * ln, ln)] = v
        for q in range(4):
            to_sib(q, y).wait_send()
            to_sib(q, 1 - y).wait_send()
            to_peer(q).wait_send()
        for q in range(2):
            to_inner(q).wait_send()

    @pl.when(jnp.logical_not(end))
    def _():
        for q in range(2):
            to_inner(q).wait_recv()
            out[pl.ds(q * ln, ln)] = rc[q]


def solution(mesh):
    tp = mesh.shape['tp']
    ep = mesh.shape['ep']
    tok_spec = P(('dp', 'tp', 'ep'), None)

    def local(x, route_idx, gates, w1, w3, w2):
        t_loc, d = x.shape
        top = route_idx.shape[1]
        e_loc, _, f = w1.shape
        n_tok = t_loc * tp * ep
        n_half = n_tok // 2
        z = lax.axis_index('tp')
        j = lax.axis_index('ep')
        side = jnp.where(z >= tp // 2, 1, 0)

        gr = t_loc * top // 128
        any_ = pl.BlockSpec(memory_space=pl.ANY)
        vmem = pl.BlockSpec(memory_space=pltpu.VMEM)
        route = jnp.pad(route_idx.astype(jnp.bfloat16), ((0, 0), (0, 128 - top)), constant_values=-1.0)
        hid, ra, ga = pl.pallas_call(
            functools.partial(hidden_kernel, tp),
            in_specs=[any_] * 5,
            out_specs=[any_] * 3,
            out_shape=[jax.ShapeDtypeStruct((n_tok, e_loc * f), x.dtype),
                       jax.ShapeDtypeStruct((tp * ep, t_loc, 128), x.dtype),
                       jax.ShapeDtypeStruct((tp * ep, gr, 128), jnp.float32)],
            scratch_shapes=[
                pltpu.VMEM((tp * ep, t_loc, d), x.dtype),
                pltpu.VMEM((tp * ep, t_loc, 128), x.dtype),
                pltpu.VMEM((tp * ep, gr, 128), jnp.float32),
                pltpu.VMEM((e_loc, d, f), x.dtype),
                pltpu.VMEM((e_loc, d, f), x.dtype),
                pltpu.VMEM((2, 4 * t_loc, e_loc * f), x.dtype),
                pltpu.SemaphoreType.DMA((3,)),
                pltpu.SemaphoreType.DMA((2, e_loc)),
                pltpu.SemaphoreType.DMA((2,)),
                pltpu.SemaphoreType.DMA((3, 5 * tp)),
                pltpu.SemaphoreType.DMA((3, tp * ep)),
            ],
            compiler_params=pltpu.CompilerParams(collective_id=20, has_side_effects=True, vmem_limit_bytes=60000 * 1024),
            name='hidden',
        )(x, route, gates.reshape(gr, 128), w1, w3)

        loc = ra.reshape(n_tok, 128)[:, :top].astype(jnp.int32) - j * e_loc
        ga = ga.reshape(n_tok, top)
        ids = jnp.arange(e_loc, dtype=jnp.int32)
        hit = jnp.any(loc.T[None] == ids[:, None, None], axis=1).reshape(e_loc, 2, n_half).transpose(1, 0, 2)
        upto = jnp.arange(n_half)[:, None] < jnp.arange(n_half)[None, :]
        pos = jnp.dot(hit.reshape(2 * e_loc, n_half).astype(jnp.bfloat16), upto.astype(jnp.bfloat16),
                      preferred_element_type=jnp.float32).astype(jnp.int32).reshape(2, e_loc, n_half)
        num = jnp.sum(hit.astype(jnp.int32), axis=2)
        off = jnp.sum(jnp.where(ids[None, :, None] > ids[None, None, :], num[:, None, :], 0), axis=2)
        total = jnp.sum(num, axis=1)
        place = off[:, :, None] + pos
        dest = jnp.where(hit, place, -1)
        full = -(-n_half * top // TC) * TC

        mine = loc.reshape(2, n_half, top)[side]
        same = mine[:, :, None] == ids[None, None, :]
        rows = jnp.sum(jnp.where(same, place[side].T[:, None, :], 0), axis=2)
        rows = jnp.where(jnp.any(same, axis=2), rows, -1)
        order = lambda v: v.reshape(tp // 2, ep, t_loc, top).transpose(1, 0, 2, 3).reshape(n_half, top)

        def chain(size, ident):
            return pl.pallas_call(
                functools.partial(chain_kernel, tp, size // BR),
                in_specs=[pl.BlockSpec(memory_space=pltpu.SMEM), vmem, vmem, vmem, any_, any_],
                out_specs=vmem,
                out_shape=jax.ShapeDtypeStruct((n_half, d), jnp.float32),
                scratch_shapes=[
                    pltpu.VMEM((n_tok, e_loc * f), x.dtype),
                    pltpu.VMEM((e_loc, f, d), x.dtype),
                    pltpu.VMEM((2, 2, TC, e_loc * f), x.dtype),
                    pltpu.VMEM((2, 3, TC, d), jnp.float32),
                    pltpu.VMEM((2, NS, BR, d), jnp.float32),
                    pltpu.VMEM((2, NS, BR, d), jnp.float32),
                    pltpu.VMEM((TC, d), jnp.bfloat16),
                    pltpu.SemaphoreType.DMA((e_loc,)),
                    pltpu.SemaphoreType.DMA((e_loc,)),
                    pltpu.SemaphoreType.DMA((2, NS)),
                    pltpu.SemaphoreType.DMA((2, NS)),
                    pltpu.SemaphoreType.REGULAR((2,)),
                ],
                compiler_params=pltpu.CompilerParams(collective_id=ident, has_side_effects=True, vmem_limit_bytes=60000 * 1024),
                name=f'chain{size}',
            )

        sizes = tuple(s for s in SIZES if s < full) + (full,)
        need = jnp.max(total)
        which = jnp.sum((need > jnp.array(sizes[:-1], jnp.int32)).astype(jnp.int32))
        py = lax.switch(which, [chain(s, i + 1) for i, s in enumerate(sizes)],
                        total[side].reshape(1), order(rows), order(ga.reshape(2, n_half, top)[side]),
                        dest.reshape(2, e_loc, 1, n_half), hid, w2)

        return pl.pallas_call(
            functools.partial(finish_kernel, tp),
            in_specs=[vmem],
            out_specs=vmem,
            out_shape=jax.ShapeDtypeStruct((t_loc, d), x.dtype),
            scratch_shapes=[
                pltpu.VMEM((2, 2 * t_loc, d), jnp.float32),
                pltpu.VMEM((2 * t_loc, d), jnp.float32),
                pltpu.VMEM((2 * t_loc, d), jnp.float32),
                pltpu.VMEM((2, t_loc // 2, d), x.dtype),
                pltpu.VMEM((2, t_loc // 2, d), x.dtype),
                pltpu.SemaphoreType.DMA((4, 2)),
                pltpu.SemaphoreType.DMA((4, 2)),
                pltpu.SemaphoreType.DMA((4,)),
                pltpu.SemaphoreType.DMA((4,)),
                pltpu.SemaphoreType.DMA((2,)),
                pltpu.SemaphoreType.DMA((2,)),
            ],
            compiler_params=pltpu.CompilerParams(collective_id=21, has_side_effects=True, vmem_limit_bytes=60000 * 1024),
            name='finish',
        )(py.reshape(ep, n_half // ep, d))

    return jax.shard_map(local, mesh=mesh,
                         in_specs=(tok_spec, tok_spec, tok_spec, P('ep', None, 'tp'), P('ep', None, 'tp'), P('ep', 'tp', None)),
                         out_specs=tok_spec, check_vma=False)
```

```python
import functools

import jax
import jax.numpy as jnp
from jax import lax
from jax.experimental import pallas as pl
from jax.experimental.pallas import tpu as pltpu
from jax.sharding import PartitionSpec as P

TM = 128
BR = 16
LAG = 3
NS = 8
NO = NS + 1
TC = 128
SIZES = (704, 832, 960, 1024, 1088, 1152, 1216, 1280, 1344, 1408, 1472, 1600, 1792, 2304)
MESH = pl.DeviceIdType.MESH


def expert_kernel(meta, dest, x, w1, w3, w2, out, obuf, carry, cnt, sem):
    e = pl.program_id(0)
    n_tok = x.shape[0]
    n_blk = TM // 8

    def copy(src, half, to, slot):
        return pltpu.make_async_copy(src, out.at[half, pl.ds(pl.multiple_of(to * 8, 8), 8)], sem.at[slot])

    def drain(slot):
        def one(_, c):
            copy(obuf.at[slot, pl.ds(0, 8)], 0, 0, slot).wait()
            return c
        lax.fori_loop(0, cnt[slot], one, 0)

    @pl.when(e == 0)
    def _():
        cnt[0] = 0
        cnt[1] = 0
        cnt[2] = 0
        carry[...] = jnp.zeros_like(carry)

    begin = (0, meta[e, 0])
    stop = (meta[e, 0], meta[e, 0] + meta[e, 1])
    place = (meta[e, 2], meta[e, 3])
    short = (meta[e, 4] > 0, meta[e, 5] > 0)
    blocks = stop[1]

    def tile(i, c):
        rows = lax.broadcasted_iota(jnp.int32, (TM, n_tok), 0) + i * TM
        pick = jnp.where(dest[0] == rows, 1.0, 0.0).astype(jnp.bfloat16)
        xs = jnp.dot(pick, x[...], preferred_element_type=jnp.float32).astype(jnp.bfloat16)
        a = jnp.dot(xs, w1[0], preferred_element_type=jnp.float32)
        b = jnp.dot(xs, w3[0], preferred_element_type=jnp.float32)
        h = (jax.nn.silu(a) * b).astype(jnp.bfloat16)
        slot = cnt[2]
        drain(slot)
        obuf[slot] = jnp.dot(h, w2[0], preferred_element_type=jnp.float32)
        low = i * n_blk
        n = jnp.minimum(n_blk, blocks - low)
        kept = jnp.int32(0)
        for half in (0, 1):
            some = stop[half] > begin[half]
            first = begin[half] - low
            final = stop[half] - 1 - low

            @pl.when(jnp.logical_and(some, jnp.logical_and(first >= 0, first < n_blk)))
            def _(half=half, first=first):
                at = pl.ds(pl.multiple_of(first * 8, 8), 8)
                obuf[slot, at] += carry[half]
                carry[half] = jnp.zeros_like(carry[half])

            keep = jnp.logical_and(jnp.logical_and(some, short[half]), jnp.logical_and(final >= 0, final < n_blk))

            @pl.when(keep)
            def _(half=half, final=final):
                carry[half] = obuf[slot, pl.ds(pl.multiple_of(final * 8, 8), 8)]
            kept = kept + jnp.where(keep, 1, 0)

        def put(k, c):
            g = low + k
            late = g >= begin[1]
            half = jnp.where(late, 1, 0)
            to = jnp.where(late, place[1] + g - begin[1], place[0] + g)
            held = jnp.where(late, jnp.logical_and(short[1], g == stop[1] - 1).astype(jnp.int32),
                             jnp.logical_and(short[0], g == stop[0] - 1).astype(jnp.int32))

            @pl.when(held == 0)
            def _():
                copy(obuf.at[slot, pl.ds(pl.multiple_of(k * 8, 8), 8)], half, to, slot).start()
            return c

        lax.fori_loop(0, n, put, 0)
        cnt[slot] = n - kept
        cnt[2] = 1 - slot
        return c

    lax.fori_loop(0, (blocks + n_blk - 1) // n_blk, tile, 0)

    @pl.when(e == pl.num_programs(0) - 1)
    def _():
        drain(0)
        drain(1)
        for half in (0, 1):
            @pl.when(meta[e, 6 + half] >= 0)
            def _(half=half):
                last = copy(carry.at[half], half, meta[e, 6 + half], 0)
                last.start()
                last.wait()


def chain_kernel(n, blocks, count, rows, gates, src, out, own, rbuf, sbuf, obuf, own_sem, send_sem, recv_sem, credit):
    z = lax.axis_index('tp')
    barrier = pltpu.get_barrier_semaphore()

    @pl.when(z > 0)
    def _():
        pl.semaphore_signal(barrier, inc=1, device_id={'tp': z - 1}, device_id_type=MESH)

    @pl.when(z < n - 1)
    def _():
        pl.semaphore_signal(barrier, inc=1, device_id={'tp': z + 1}, device_id_type=MESH)

    pl.semaphore_wait(barrier, jnp.where(z > 0, 1, 0) + jnp.where(z < n - 1, 1, 0))

    def load(d, k):
        s = lax.rem(k, NO)
        return pltpu.make_async_copy(src.at[1 - d, pl.ds(pl.multiple_of(k * BR, BR), BR)], own.at[d, s], own_sem.at[d, s])

    def send(d, k, buf, s_buf):
        s = lax.rem(k, NS)
        to = z + 1 if d == 0 else z - 1
        return pltpu.make_async_remote_copy(
            src_ref=buf.at[d, s_buf], dst_ref=rbuf.at[d, s], send_sem=send_sem.at[d, s], recv_sem=recv_sem.at[d, s],
            device_id={'tp': to}, device_id_type=MESH)

    per = TC // BR

    def gated(j):
        col = lax.broadcasted_iota(jnp.int32, (rows.shape[0], TC), 1) + j * TC
        g = jnp.zeros((rows.shape[0], TC), jnp.float32)
        for k in range(rows.shape[1]):
            g = g + jnp.where(rows[:, k:k + 1] == col, gates[:, k:k + 1], 0.0)
        g1 = g.astype(jnp.bfloat16)
        rest = g - g1.astype(jnp.float32)
        g2 = rest.astype(jnp.bfloat16)
        g3 = (rest - g2.astype(jnp.float32)).astype(jnp.bfloat16)
        g = jnp.concatenate([g1, g2, g3], axis=1)
        wide = min(256, out.shape[1])
        row = lax.broadcasted_iota(jnp.int32, (TC, wide), 0) + j * TC

        def columns(q, c):
            at = pl.ds(pl.multiple_of(q * wide, wide), wide)
            o = jnp.where(row < count[0], obuf[:, at].astype(jnp.float32), 0.0).astype(jnp.bfloat16)
            out[:, at] += jnp.dot(g, jnp.concatenate([o, o, o], axis=0), preferred_element_type=jnp.float32)
            return c

        lax.fori_loop(0, out.shape[1] // wide, columns, 0)

    def step(i, c):
        work = []
        for d in (0, 1):
            p = z if d == 0 else n - 1 - z
            k = i - LAG * p
            work.append((d, p, k, jnp.logical_and(k >= 0, k < blocks)))

        for d, p, k, live in work:
            @pl.when(live)
            def _(d=d, p=p, k=k):
                @pl.when(jnp.logical_and(p < n - 1, k >= NS))
                def _():
                    send(d, k - NS, sbuf, lax.rem(k, NS)).wait_send()

                @pl.when(k == 0)
                def _():
                    load(d, k).start()

                @pl.when(k + 1 < blocks)
                def _():
                    load(d, k + 1).start()

                load(d, k).wait()

        for d, p, k, live in work:
            @pl.when(jnp.logical_and(live, p == 0))
            def _(d=d, k=k):
                @pl.when(k >= NS)
                def _():
                    pl.semaphore_wait(credit.at[d], 1)
                send(d, k, own, lax.rem(k, NO)).start()

        for d, p, k, live in work:
            @pl.when(jnp.logical_and(live, p > 0))
            def _(d=d, p=p, k=k):
                s = lax.rem(k, NS)
                send(d, k, sbuf, s).wait_recv()

                @pl.when(p < n - 1)
                def _():
                    sbuf[d, s] = rbuf[d, s] + own[d, lax.rem(k, NO)]

                @pl.when(p == n - 1)
                def _():
                    to = pl.multiple_of(lax.rem(k, per) * BR, BR)
                    obuf[pl.ds(to, BR)] = (rbuf[d, s] + own[d, lax.rem(k, NO)]).astype(jnp.bfloat16)

                @pl.when(k + NS < blocks)
                def _():
                    back = z - 1 if d == 0 else z + 1
                    pl.semaphore_signal(credit.at[d], inc=1, device_id={'tp': back}, device_id_type=MESH)

        for d, p, k, live in work:
            @pl.when(jnp.logical_and(live, jnp.logical_and(p > 0, p < n - 1)))
            def _(d=d, k=k):
                @pl.when(k >= NS)
                def _():
                    pl.semaphore_wait(credit.at[d], 1)
                send(d, k, sbuf, lax.rem(k, NS)).start()

        k = i - LAG * (n - 1)

        @pl.when(jnp.logical_and(jnp.logical_or(z == 0, z == n - 1), jnp.logical_and(k >= 0, jnp.logical_or(lax.rem(k + per, per) == per - 1, k == blocks - 1))))
        def _():
            gated(k // per)
        return c

    @pl.when(jnp.logical_or(z == 0, z == n - 1))
    def _():
        out[...] = jnp.zeros_like(out)

    lax.fori_loop(0, blocks + LAG * (n - 1), step, 0)

    for d in (0, 1):
        p = z if d == 0 else n - 1 - z

        @pl.when(p < n - 1)
        def _(d=d):
            for k in range(blocks - NS, blocks):
                send(d, k, sbuf, k % NS).wait_send()


def gather_kernel(n, x, info, xout, iout, xbuf, ibuf, own_sem, xsend, isend, xrecv, irecv, out_sem):
    z = lax.axis_index('tp')
    j = lax.axis_index('ep')
    t_loc = x.shape[0]
    sib = j + 1 - 2 * lax.rem(j, 2)
    peer = lax.rem(j + 2, 4)
    blk = lambda zz, jj: zz * 4 + jj
    up, down = {'tp': z + 1}, {'tp': z - 1}
    me = blk(z, j)
    mine = (pltpu.make_async_copy(x, xbuf.at[me], own_sem.at[0]), pltpu.make_async_copy(info, ibuf.at[me], own_sem.at[1]))
    for m in mine:
        m.start()

    barrier = pltpu.get_barrier_semaphore()
    for other in (sib, peer):
        pl.semaphore_signal(barrier, inc=1, device_id={'ep': other}, device_id_type=MESH)

    @pl.when(z > 0)
    def _():
        pl.semaphore_signal(barrier, inc=1, device_id=down, device_id_type=MESH)

    @pl.when(z < n - 1)
    def _():
        pl.semaphore_signal(barrier, inc=1, device_id=up, device_id_type=MESH)

    pl.semaphore_wait(barrier, 2 + jnp.where(z > 0, 1, 0) + jnp.where(z < n - 1, 1, 0))

    def copies(b, i, dev):
        make = lambda buf, s, r: pltpu.make_async_remote_copy(
            src_ref=buf.at[b], dst_ref=buf.at[b], send_sem=s.at[i], recv_sem=r.at[b], device_id=dev, device_id_type=MESH)
        return make(ibuf, isend, irecv), make(xbuf, xsend, xrecv)

    def send(b, i, dev):
        for c in copies(b, i, dev):
            c.start()

    def sent(b, i, dev):
        for c in copies(b, i, dev):
            c.wait_send()

    def arrive(b):
        for c in copies(b, 0, {'ep': sib}):
            c.wait_recv()

    def keep(b):
        return pltpu.make_async_copy(xbuf.at[b], xout.at[pl.ds(pl.multiple_of(b * t_loc, t_loc), t_loc)], out_sem.at[b])

    def line(f):
        f(z, 0, True, True)
        for r in range(1, n):
            @pl.when(z >= r)
            def _(r=r):
                f(z - r, r, True, False)

            @pl.when(z + r < n)
            def _(r=r):
                f(z + r, r, False, True)

    def spread(act):
        def f(zz, r, ups, downs):
            b = blk(zz, j)
            if act is send:
                if r == 0:
                    for m in mine:
                        m.wait()
                else:
                    arrive(b)
            if ups:
                @pl.when(z < n - 1)
                def _():
                    act(b, r, up)
            if downs:
                @pl.when(z > 0)
                def _():
                    act(b, n + r, down)
            act(b, 2 * n + zz, {'ep': peer})
            act(b, 3 * n + zz, {'ep': sib})
            if act is send:
                keep(b).start()
        return f

    def relay(act):
        def f(zz, r, ups, downs):
            b = blk(zz, peer)
            if act is send:
                arrive(b)
            act(b, 4 * n + zz, {'ep': sib})
            if act is send:
                keep(b).start()
        return f

    line(spread(send))
    line(relay(send))
    for other in (sib, lax.rem(sib + 2, 4)):
        def take(zz, r, ups, downs, other=other):
            arrive(blk(zz, other))
            keep(blk(zz, other)).start()
        line(take)
    every = pltpu.make_async_copy(ibuf, iout, own_sem.at[0])
    every.start()
    line(spread(sent))
    line(relay(sent))
    for b in range(4 * n):
        keep(b).wait()
    every.wait()


def finish_kernel(n, py, out, ra, sb, rb, yb, rc, a_send, a_recv, b_send, b_recv, c_send, c_recv):
    z = lax.axis_index('tp')
    j = lax.axis_index('ep')
    t_loc = out.shape[0]
    ln = t_loc // 2
    y, c = j // 2, lax.rem(j, 2)
    sib = j + 1 - 2 * c
    peer = lax.rem(j + 2, 4)
    end = jnp.logical_or(z == 0, z == n - 1)
    low = z < n // 2
    across = jnp.where(z == 0, 1, jnp.where(z == 1, 0, jnp.where(z == n - 1, n - 2, n - 1)))
    barrier = pltpu.get_barrier_semaphore()
    pl.semaphore_signal(barrier, inc=1, device_id={'tp': across}, device_id_type=MESH)

    @pl.when(end)
    def _():
        for other in (sib, peer):
            pl.semaphore_signal(barrier, inc=1, device_id={'ep': other}, device_id_type=MESH)

    pl.semaphore_wait(barrier, jnp.where(end, 3, 1))

    inner = jnp.where(low, 1, 0)
    starts = [pl.multiple_of((inner if q < 2 else 1 - inner) * t_loc + (q % 2) * ln, ln) for q in range(4)]

    def to_sib(q, yy):
        at = pl.ds(starts[q], ln)
        return pltpu.make_async_remote_copy(
            src_ref=py.at[2 * yy + 1 - c, at], dst_ref=ra.at[yy, at], send_sem=a_send.at[q, yy], recv_sem=a_recv.at[q, yy],
            device_id={'ep': sib}, device_id_type=MESH)

    def to_peer(q):
        at = pl.ds(starts[q], ln)
        return pltpu.make_async_remote_copy(
            src_ref=sb.at[at], dst_ref=rb.at[at], send_sem=b_send.at[q], recv_sem=b_recv.at[q],
            device_id={'ep': peer}, device_id_type=MESH)

    def to_inner(q):
        return pltpu.make_async_remote_copy(
            src_ref=yb.at[q], dst_ref=rc.at[q], send_sem=c_send.at[q], recv_sem=c_recv.at[q],
            device_id={'tp': across}, device_id_type=MESH)

    @pl.when(end)
    def _():
        for q in range(4):
            to_sib(q, 1 - y).start()
        for q in range(4):
            to_sib(q, y).start()
        for q in range(4):
            at = pl.ds(starts[q], ln)
            to_sib(q, 1 - y).wait_recv()
            sb[at] = py[2 * (1 - y) + c, at] + ra[1 - y, at]
            to_peer(q).start()
        for q in range(4):
            at = pl.ds(starts[q], ln)
            to_sib(q, y).wait_recv()
            to_peer(q).wait_recv()
            v = ((py[2 * y + c, at] + ra[y, at]) + rb[at]).astype(jnp.bfloat16)
            if q < 2:
                yb[q] = v
                to_inner(q).start()
            else:
                out[pl.ds((q - 2) * ln, ln)] = v
        for q in range(4):
            to_sib(q, y).wait_send()
            to_sib(q, 1 - y).wait_send()
            to_peer(q).wait_send()
        for q in range(2):
            to_inner(q).wait_send()

    @pl.when(jnp.logical_not(end))
    def _():
        for q in range(2):
            to_inner(q).wait_recv()
            out[pl.ds(q * ln, ln)] = rc[q]


def solution(mesh):
    tp = mesh.shape['tp']
    ep = mesh.shape['ep']
    tok_spec = P(('dp', 'tp', 'ep'), None)

    def local(x, route_idx, gates, w1, w3, w2):
        t_loc, d = x.shape
        top = route_idx.shape[1]
        e_loc, _, f = w1.shape
        n_tok = t_loc * tp * ep
        n_half = n_tok // 2
        z = lax.axis_index('tp')
        j = lax.axis_index('ep')
        side = jnp.where(z >= tp // 2, 1, 0)

        own = jnp.concatenate([route_idx.astype(jnp.float32), gates], axis=1)
        ir = t_loc * 2 * top // 128
        any_ = pl.BlockSpec(memory_space=pl.ANY)
        vmem = pl.BlockSpec(memory_space=pltpu.VMEM)
        xa, info = pl.pallas_call(
            functools.partial(gather_kernel, tp),
            in_specs=[any_, any_],
            out_specs=[any_, any_],
            out_shape=[jax.ShapeDtypeStruct((n_tok, d), x.dtype), jax.ShapeDtypeStruct((tp * ep, ir, 128), jnp.float32)],
            scratch_shapes=[
                pltpu.VMEM((tp * ep, t_loc, d), x.dtype),
                pltpu.VMEM((tp * ep, ir, 128), jnp.float32),
                pltpu.SemaphoreType.DMA((2,)),
                pltpu.SemaphoreType.DMA((5 * tp,)),
                pltpu.SemaphoreType.DMA((5 * tp,)),
                pltpu.SemaphoreType.DMA((tp * ep,)),
                pltpu.SemaphoreType.DMA((tp * ep,)),
                pltpu.SemaphoreType.DMA((tp * ep,)),
            ],
            compiler_params=pltpu.CompilerParams(collective_id=20, has_side_effects=True),
            name='gather',
        )(x, own.reshape(ir, 128))
        info = info.reshape(n_tok, 2 * top)

        loc = info[:, :top].astype(jnp.int32) - j * e_loc
        ga = info[:, top:]
        ids = jnp.arange(e_loc, dtype=jnp.int32)
        hit = jnp.any(loc.T[None] == ids[:, None, None], axis=1)
        before = jnp.arange(n_half)[:, None] < jnp.arange(n_half)[None, :]
        hit2 = hit.reshape(e_loc * 2, n_half)
        pos = jnp.dot(hit2.astype(jnp.bfloat16), before.astype(jnp.bfloat16),
                      preferred_element_type=jnp.float32).astype(jnp.int32).reshape(e_loc, 2, n_half)
        n = jnp.sum(hit2.astype(jnp.int32), axis=1).reshape(e_loc, 2)
        off = jnp.sum(jnp.where(ids[:, None, None] > ids[None, :, None], n[None], 0), axis=1)
        total = jnp.sum(n, axis=0)
        lead = off % 8
        nb = jnp.where(n > 0, (lead + n + 7) // 8, 0)
        left = jnp.broadcast_to(jnp.where(total % 8 > 0, total // 8, -1)[None], (e_loc, 2))
        meta = jnp.concatenate([nb, off // 8, (off + n) % 8, left], axis=1)
        base = jnp.stack([lead[:, 0], nb[:, 0] * 8 + lead[:, 1]], axis=1)
        dest = jnp.where(hit, (base[:, :, None] + pos).reshape(e_loc, n_tok), -1)

        full = -(-n_half * top // TC) * TC
        part = pl.pallas_call(
            expert_kernel,
            grid_spec=pltpu.PrefetchScalarGridSpec(
                num_scalar_prefetch=1,
                grid=(e_loc,),
                in_specs=[
                    pl.BlockSpec((1, 1, n_tok), lambda e, m: (e, 0, 0)),
                    pl.BlockSpec((n_tok, d), lambda e, m: (0, 0)),
                    pl.BlockSpec((1, d, f), lambda e, m: (e, 0, 0)),
                    pl.BlockSpec((1, d, f), lambda e, m: (e, 0, 0)),
                    pl.BlockSpec((1, f, d), lambda e, m: (e, 0, 0)),
                ],
                out_specs=pl.BlockSpec(memory_space=pl.ANY),
                scratch_shapes=[
                    pltpu.VMEM((2, TM, d), jnp.float32),
                    pltpu.VMEM((2, 8, d), jnp.float32),
                    pltpu.SMEM((3,), jnp.int32),
                    pltpu.SemaphoreType.DMA((2,)),
                ]),
            out_shape=jax.ShapeDtypeStruct((2, full, d), jnp.float32),
            compiler_params=pltpu.CompilerParams(dimension_semantics=('arbitrary',), vmem_limit_bytes=60000 * 1024),
            name='experts',
        )(meta, dest.reshape(e_loc, 1, n_tok), xa, w1, w3, w2)

        row = (off[:, :, None] + pos)[:, side]
        mine = loc.reshape(2, n_half, top)[side]
        same = mine[:, :, None] == ids[None, None, :]
        rows = jnp.sum(jnp.where(same, row.T[:, None, :], 0), axis=2)
        rows = jnp.where(jnp.any(same, axis=2), rows, -1)
        order = lambda v: v.reshape(tp // 2, ep, t_loc, top).transpose(1, 0, 2, 3).reshape(n_half, top)

        def chain(size, ident):
            return pl.pallas_call(
                functools.partial(chain_kernel, tp, size // BR),
                in_specs=[pl.BlockSpec(memory_space=pltpu.SMEM), vmem, vmem, any_],
                out_specs=vmem,
                out_shape=jax.ShapeDtypeStruct((n_half, d), jnp.float32),
                scratch_shapes=[
                    pltpu.VMEM((2, NO, BR, d), jnp.float32),
                    pltpu.VMEM((2, NS, BR, d), jnp.float32),
                    pltpu.VMEM((2, NS, BR, d), jnp.float32),
                    pltpu.VMEM((TC, d), jnp.bfloat16),
                    pltpu.SemaphoreType.DMA((2, NO)),
                    pltpu.SemaphoreType.DMA((2, NS)),
                    pltpu.SemaphoreType.DMA((2, NS)),
                    pltpu.SemaphoreType.REGULAR((2,)),
                ],
                compiler_params=pltpu.CompilerParams(collective_id=ident, has_side_effects=True, vmem_limit_bytes=60000 * 1024),
                name=f'chain{size}',
            )

        sizes = tuple(s for s in SIZES if s < full) + (full,)
        need = jnp.max(total)
        which = jnp.sum((need > jnp.array(sizes[:-1], jnp.int32)).astype(jnp.int32))
        py = lax.switch(which, [chain(s, i + 1) for i, s in enumerate(sizes)],
                        total[side].reshape(1), order(rows), order(ga.reshape(2, n_half, top)[side]), part)

        return pl.pallas_call(
            functools.partial(finish_kernel, tp),
            in_specs=[vmem],
            out_specs=vmem,
            out_shape=jax.ShapeDtypeStruct((t_loc, d), x.dtype),
            scratch_shapes=[
                pltpu.VMEM((2, 2 * t_loc, d), jnp.float32),
                pltpu.VMEM((2 * t_loc, d), jnp.float32),
                pltpu.VMEM((2 * t_loc, d), jnp.float32),
                pltpu.VMEM((2, t_loc // 2, d), x.dtype),
                pltpu.VMEM((2, t_loc // 2, d), x.dtype),
                pltpu.SemaphoreType.DMA((4, 2)),
                pltpu.SemaphoreType.DMA((4, 2)),
                pltpu.SemaphoreType.DMA((4,)),
                pltpu.SemaphoreType.DMA((4,)),
                pltpu.SemaphoreType.DMA((2,)),
                pltpu.SemaphoreType.DMA((2,)),
            ],
            compiler_params=pltpu.CompilerParams(collective_id=21, has_side_effects=True, vmem_limit_bytes=60000 * 1024),
            name='finish',
        )(py.reshape(ep, n_half // ep, d))

    return jax.shard_map(local, mesh=mesh,
                         in_specs=(tok_spec, tok_spec, tok_spec, P('ep', None, 'tp'), P('ep', None, 'tp'), P('ep', 'tp', None)),
                         out_specs=tok_spec, check_vma=False)
```

```python
import functools

import jax
import jax.numpy as jnp
from jax import lax
from jax.experimental import pallas as pl
from jax.experimental.pallas import tpu as pltpu
from jax.sharding import PartitionSpec as P

TM = 128
BR = 16
LAG = 3
NS = 8
NO = NS + 1
TC = 128
SIZES = (832, 960, 1024, 1088, 1152, 1216, 1280, 1344, 1408, 1472, 1600, 1792, 2304)
MESH = pl.DeviceIdType.MESH


def expert_kernel(meta, dest, x, w1, w3, w2, out, obuf, carry, xbuf, cnt, sem):
    e = pl.program_id(0)
    n_tok = x.shape[0]
    n_blk = TM // 8

    def copy(src, half, to, slot):
        return pltpu.make_async_copy(src, out.at[half, pl.ds(pl.multiple_of(to * 8, 8), 8)], sem.at[slot])

    def drain(slot):
        def one(_, c):
            copy(obuf.at[slot, pl.ds(0, 8)], 0, 0, slot).wait()
            return c
        lax.fori_loop(0, cnt[slot], one, 0)

    def fetch(who, i, s):
        rows = lax.broadcasted_iota(jnp.int32, (TM, n_tok), 0) + i * TM
        pick = jnp.where(dest[who] == rows, 1.0, 0.0).astype(jnp.bfloat16)
        xbuf[s] = jnp.dot(pick, x[...], preferred_element_type=jnp.float32).astype(jnp.bfloat16)

    after = jnp.minimum(e + 1, pl.num_programs(0) - 1)

    @pl.when(e == 0)
    def _():
        cnt[0] = 0
        cnt[1] = 0
        cnt[2] = 0
        cnt[3] = 0
        carry[...] = jnp.zeros_like(carry)
        fetch(0, 0, 0)

    begin = (0, meta[e, 0])
    stop = (meta[e, 0], meta[e, 0] + meta[e, 1])
    place = (meta[e, 2], meta[e, 3])
    short = (meta[e, 4] > 0, meta[e, 5] > 0)
    blocks = stop[1]
    tiles = (blocks + n_blk - 1) // n_blk

    @pl.when(tiles == 0)
    def _():
        fetch(after, 0, cnt[3])

    def tile(i, c):
        slot, s = cnt[2], cnt[3]
        drain(slot)
        xs = xbuf[s]
        a = jnp.dot(xs, w1[0], preferred_element_type=jnp.float32)
        b = jnp.dot(xs, w3[0], preferred_element_type=jnp.float32)
        h = (jax.nn.silu(a) * b).astype(jnp.bfloat16)
        obuf[slot] = jnp.dot(h, w2[0], preferred_element_type=jnp.float32)
        more = i + 1 < tiles
        fetch(jnp.where(more, e, after), jnp.where(more, i + 1, 0), 1 - s)
        cnt[3] = 1 - s
        low = i * n_blk
        n = jnp.minimum(n_blk, blocks - low)
        kept = jnp.int32(0)
        for half in (0, 1):
            some = stop[half] > begin[half]
            first = begin[half] - low
            final = stop[half] - 1 - low

            @pl.when(jnp.logical_and(some, jnp.logical_and(first >= 0, first < n_blk)))
            def _(half=half, first=first):
                at = pl.ds(pl.multiple_of(first * 8, 8), 8)
                obuf[slot, at] += carry[half]
                carry[half] = jnp.zeros_like(carry[half])

            keep = jnp.logical_and(jnp.logical_and(some, short[half]), jnp.logical_and(final >= 0, final < n_blk))

            @pl.when(keep)
            def _(half=half, final=final):
                carry[half] = obuf[slot, pl.ds(pl.multiple_of(final * 8, 8), 8)]
            kept = kept + jnp.where(keep, 1, 0)

        def put(k, c):
            g = low + k
            late = g >= begin[1]
            half = jnp.where(late, 1, 0)
            to = jnp.where(late, place[1] + g - begin[1], place[0] + g)
            held = jnp.where(late, jnp.logical_and(short[1], g == stop[1] - 1).astype(jnp.int32),
                             jnp.logical_and(short[0], g == stop[0] - 1).astype(jnp.int32))

            @pl.when(held == 0)
            def _():
                copy(obuf.at[slot, pl.ds(pl.multiple_of(k * 8, 8), 8)], half, to, slot).start()
            return c

        lax.fori_loop(0, n, put, 0)
        cnt[slot] = n - kept
        cnt[2] = 1 - slot
        return c

    lax.fori_loop(0, tiles, tile, 0)

    @pl.when(e == pl.num_programs(0) - 1)
    def _():
        drain(0)
        drain(1)
        for half in (0, 1):
            @pl.when(meta[e, 6 + half] >= 0)
            def _(half=half):
                last = copy(carry.at[half], half, meta[e, 6 + half], 0)
                last.start()
                last.wait()


def chain_kernel(n, blocks, count, rows, gates, src, out, own, rbuf, sbuf, obuf, own_sem, send_sem, recv_sem, credit):
    z = lax.axis_index('tp')
    barrier = pltpu.get_barrier_semaphore()

    @pl.when(z > 0)
    def _():
        pl.semaphore_signal(barrier, inc=1, device_id={'tp': z - 1}, device_id_type=MESH)

    @pl.when(z < n - 1)
    def _():
        pl.semaphore_signal(barrier, inc=1, device_id={'tp': z + 1}, device_id_type=MESH)

    pl.semaphore_wait(barrier, jnp.where(z > 0, 1, 0) + jnp.where(z < n - 1, 1, 0))

    def load(d, k):
        s = lax.rem(k, NO)
        return pltpu.make_async_copy(src.at[1 - d, pl.ds(pl.multiple_of(k * BR, BR), BR)], own.at[d, s], own_sem.at[d, s])

    def send(d, k, buf, s_buf):
        s = lax.rem(k, NS)
        to = z + 1 if d == 0 else z - 1
        return pltpu.make_async_remote_copy(
            src_ref=buf.at[d, s_buf], dst_ref=rbuf.at[d, s], send_sem=send_sem.at[d, s], recv_sem=recv_sem.at[d, s],
            device_id={'tp': to}, device_id_type=MESH)

    per = TC // BR

    def gated(j):
        col = lax.broadcasted_iota(jnp.int32, (rows.shape[0], TC), 1) + j * TC
        g = jnp.zeros((rows.shape[0], TC), jnp.float32)
        for k in range(rows.shape[1]):
            g = g + jnp.where(rows[:, k:k + 1] == col, gates[:, k:k + 1], 0.0)
        g1 = g.astype(jnp.bfloat16)
        rest = g - g1.astype(jnp.float32)
        g2 = rest.astype(jnp.bfloat16)
        g3 = (rest - g2.astype(jnp.float32)).astype(jnp.bfloat16)
        g = jnp.concatenate([g1, g2, g3], axis=1)
        wide = min(256, out.shape[1])
        row = lax.broadcasted_iota(jnp.int32, (TC, wide), 0) + j * TC

        def columns(q, c):
            at = pl.ds(pl.multiple_of(q * wide, wide), wide)
            o = jnp.where(row < count[0], obuf[:, at].astype(jnp.float32), 0.0).astype(jnp.bfloat16)
            out[:, at] += jnp.dot(g, jnp.concatenate([o, o, o], axis=0), preferred_element_type=jnp.float32)
            return c

        lax.fori_loop(0, out.shape[1] // wide, columns, 0)

    def step(i, c):
        work = []
        for d in (0, 1):
            p = z if d == 0 else n - 1 - z
            k = i - LAG * p
            work.append((d, p, k, jnp.logical_and(k >= 0, k < blocks)))

        for d, p, k, live in work:
            @pl.when(live)
            def _(d=d, p=p, k=k):
                @pl.when(jnp.logical_and(p < n - 1, k >= NS))
                def _():
                    send(d, k - NS, sbuf, lax.rem(k, NS)).wait_send()

                @pl.when(k == 0)
                def _():
                    load(d, k).start()

                @pl.when(k + 1 < blocks)
                def _():
                    load(d, k + 1).start()

                load(d, k).wait()

        for d, p, k, live in work:
            @pl.when(jnp.logical_and(live, p == 0))
            def _(d=d, k=k):
                @pl.when(k >= NS)
                def _():
                    pl.semaphore_wait(credit.at[d], 1)
                send(d, k, own, lax.rem(k, NO)).start()

        for d, p, k, live in work:
            @pl.when(jnp.logical_and(live, p > 0))
            def _(d=d, p=p, k=k):
                s = lax.rem(k, NS)
                send(d, k, sbuf, s).wait_recv()

                @pl.when(p < n - 1)
                def _():
                    sbuf[d, s] = rbuf[d, s] + own[d, lax.rem(k, NO)]

                @pl.when(p == n - 1)
                def _():
                    to = pl.multiple_of(lax.rem(k, per) * BR, BR)
                    obuf[pl.ds(to, BR)] = (rbuf[d, s] + own[d, lax.rem(k, NO)]).astype(jnp.bfloat16)

                @pl.when(k + NS < blocks)
                def _():
                    back = z - 1 if d == 0 else z + 1
                    pl.semaphore_signal(credit.at[d], inc=1, device_id={'tp': back}, device_id_type=MESH)

        for d, p, k, live in work:
            @pl.when(jnp.logical_and(live, jnp.logical_and(p > 0, p < n - 1)))
            def _(d=d, k=k):
                @pl.when(k >= NS)
                def _():
                    pl.semaphore_wait(credit.at[d], 1)
                send(d, k, sbuf, lax.rem(k, NS)).start()

        k = i - LAG * (n - 1)

        @pl.when(jnp.logical_and(jnp.logical_or(z == 0, z == n - 1), jnp.logical_and(k >= 0, jnp.logical_or(lax.rem(k + per, per) == per - 1, k == blocks - 1))))
        def _():
            gated(k // per)
        return c

    @pl.when(jnp.logical_or(z == 0, z == n - 1))
    def _():
        out[...] = jnp.zeros_like(out)

    lax.fori_loop(0, blocks + LAG * (n - 1), step, 0)

    for d in (0, 1):
        p = z if d == 0 else n - 1 - z

        @pl.when(p < n - 1)
        def _(d=d):
            for k in range(blocks - NS, blocks):
                send(d, k, sbuf, k % NS).wait_send()


def gather_kernel(n, x, info, xout, iout, xbuf, ibuf, own_sem, xsend, isend, xrecv, irecv, out_sem):
    z = lax.axis_index('tp')
    j = lax.axis_index('ep')
    t_loc = x.shape[0]
    sib = j + 1 - 2 * lax.rem(j, 2)
    peer = lax.rem(j + 2, 4)
    blk = lambda zz, jj: zz * 4 + jj
    up, down = {'tp': z + 1}, {'tp': z - 1}
    me = blk(z, j)
    mine = (pltpu.make_async_copy(x, xbuf.at[me], own_sem.at[0]), pltpu.make_async_copy(info, ibuf.at[me], own_sem.at[1]))
    for m in mine:
        m.start()

    barrier = pltpu.get_barrier_semaphore()
    for other in (sib, peer):
        pl.semaphore_signal(barrier, inc=1, device_id={'ep': other}, device_id_type=MESH)

    @pl.when(z > 0)
    def _():
        pl.semaphore_signal(barrier, inc=1, device_id=down, device_id_type=MESH)

    @pl.when(z < n - 1)
    def _():
        pl.semaphore_signal(barrier, inc=1, device_id=up, device_id_type=MESH)

    pl.semaphore_wait(barrier, 2 + jnp.where(z > 0, 1, 0) + jnp.where(z < n - 1, 1, 0))

    def copies(b, i, dev):
        make = lambda buf, s, r: pltpu.make_async_remote_copy(
            src_ref=buf.at[b], dst_ref=buf.at[b], send_sem=s.at[i], recv_sem=r.at[b], device_id=dev, device_id_type=MESH)
        return make(ibuf, isend, irecv), make(xbuf, xsend, xrecv)

    def send(b, i, dev):
        for c in copies(b, i, dev):
            c.start()

    def sent(b, i, dev):
        for c in copies(b, i, dev):
            c.wait_send()

    def arrive(b):
        for c in copies(b, 0, {'ep': sib}):
            c.wait_recv()

    def keep(b):
        return pltpu.make_async_copy(xbuf.at[b], xout.at[pl.ds(pl.multiple_of(b * t_loc, t_loc), t_loc)], out_sem.at[b])

    def line(f):
        f(z, 0, True, True)
        for r in range(1, n):
            @pl.when(z >= r)
            def _(r=r):
                f(z - r, r, True, False)

            @pl.when(z + r < n)
            def _(r=r):
                f(z + r, r, False, True)

    def spread(act):
        def f(zz, r, ups, downs):
            b = blk(zz, j)
            if act is send:
                if r == 0:
                    for m in mine:
                        m.wait()
                else:
                    arrive(b)
            if ups:
                @pl.when(z < n - 1)
                def _():
                    act(b, r, up)
            if downs:
                @pl.when(z > 0)
                def _():
                    act(b, n + r, down)
            act(b, 2 * n + zz, {'ep': peer})
            act(b, 3 * n + zz, {'ep': sib})
            if act is send:
                keep(b).start()
        return f

    def relay(act):
        def f(zz, r, ups, downs):
            b = blk(zz, peer)
            if act is send:
                arrive(b)
            act(b, 4 * n + zz, {'ep': sib})
            if act is send:
                keep(b).start()
        return f

    line(spread(send))
    line(relay(send))
    for other in (sib, lax.rem(sib + 2, 4)):
        def take(zz, r, ups, downs, other=other):
            arrive(blk(zz, other))
            keep(blk(zz, other)).start()
        line(take)
    every = pltpu.make_async_copy(ibuf, iout, own_sem.at[0])
    every.start()
    line(spread(sent))
    line(relay(sent))
    for b in range(4 * n):
        keep(b).wait()
    every.wait()


def finish_kernel(n, py, out, ra, sb, rb, yb, rc, a_send, a_recv, b_send, b_recv, c_send, c_recv):
    z = lax.axis_index('tp')
    j = lax.axis_index('ep')
    t_loc = out.shape[0]
    ln = t_loc // 2
    y, c = j // 2, lax.rem(j, 2)
    sib = j + 1 - 2 * c
    peer = lax.rem(j + 2, 4)
    end = jnp.logical_or(z == 0, z == n - 1)
    low = z < n // 2
    across = jnp.where(z == 0, 1, jnp.where(z == 1, 0, jnp.where(z == n - 1, n - 2, n - 1)))
    barrier = pltpu.get_barrier_semaphore()
    pl.semaphore_signal(barrier, inc=1, device_id={'tp': across}, device_id_type=MESH)

    @pl.when(end)
    def _():
        for other in (sib, peer):
            pl.semaphore_signal(barrier, inc=1, device_id={'ep': other}, device_id_type=MESH)

    pl.semaphore_wait(barrier, jnp.where(end, 3, 1))

    inner = jnp.where(low, 1, 0)
    starts = [pl.multiple_of((inner if q < 2 else 1 - inner) * t_loc + (q % 2) * ln, ln) for q in range(4)]

    def to_sib(q, yy):
        at = pl.ds(starts[q], ln)
        return pltpu.make_async_remote_copy(
            src_ref=py.at[2 * yy + 1 - c, at], dst_ref=ra.at[yy, at], send_sem=a_send.at[q, yy], recv_sem=a_recv.at[q, yy],
            device_id={'ep': sib}, device_id_type=MESH)

    def to_peer(q):
        at = pl.ds(starts[q], ln)
        return pltpu.make_async_remote_copy(
            src_ref=sb.at[at], dst_ref=rb.at[at], send_sem=b_send.at[q], recv_sem=b_recv.at[q],
            device_id={'ep': peer}, device_id_type=MESH)

    def to_inner(q):
        return pltpu.make_async_remote_copy(
            src_ref=yb.at[q], dst_ref=rc.at[q], send_sem=c_send.at[q], recv_sem=c_recv.at[q],
            device_id={'tp': across}, device_id_type=MESH)

    @pl.when(end)
    def _():
        for q in range(4):
            to_sib(q, 1 - y).start()
        for q in range(4):
            to_sib(q, y).start()
        for q in range(4):
            at = pl.ds(starts[q], ln)
            to_sib(q, 1 - y).wait_recv()
            sb[at] = py[2 * (1 - y) + c, at] + ra[1 - y, at]
            to_peer(q).start()
        for q in range(4):
            at = pl.ds(starts[q], ln)
            to_sib(q, y).wait_recv()
            to_peer(q).wait_recv()
            v = ((py[2 * y + c, at] + ra[y, at]) + rb[at]).astype(jnp.bfloat16)
            if q < 2:
                yb[q] = v
                to_inner(q).start()
            else:
                out[pl.ds((q - 2) * ln, ln)] = v
        for q in range(4):
            to_sib(q, y).wait_send()
            to_sib(q, 1 - y).wait_send()
            to_peer(q).wait_send()
        for q in range(2):
            to_inner(q).wait_send()

    @pl.when(jnp.logical_not(end))
    def _():
        for q in range(2):
            to_inner(q).wait_recv()
            out[pl.ds(q * ln, ln)] = rc[q]


def solution(mesh):
    tp = mesh.shape['tp']
    ep = mesh.shape['ep']
    tok_spec = P(('dp', 'tp', 'ep'), None)

    def local(x, route_idx, gates, w1, w3, w2):
        t_loc, d = x.shape
        top = route_idx.shape[1]
        e_loc, _, f = w1.shape
        n_tok = t_loc * tp * ep
        n_half = n_tok // 2
        z = lax.axis_index('tp')
        j = lax.axis_index('ep')
        side = jnp.where(z >= tp // 2, 1, 0)

        own = jnp.concatenate([route_idx.astype(jnp.float32), gates], axis=1)
        ir = t_loc * 2 * top // 128
        any_ = pl.BlockSpec(memory_space=pl.ANY)
        vmem = pl.BlockSpec(memory_space=pltpu.VMEM)
        xa, info = pl.pallas_call(
            functools.partial(gather_kernel, tp),
            in_specs=[any_, any_],
            out_specs=[any_, any_],
            out_shape=[jax.ShapeDtypeStruct((n_tok, d), x.dtype), jax.ShapeDtypeStruct((tp * ep, ir, 128), jnp.float32)],
            scratch_shapes=[
                pltpu.VMEM((tp * ep, t_loc, d), x.dtype),
                pltpu.VMEM((tp * ep, ir, 128), jnp.float32),
                pltpu.SemaphoreType.DMA((2,)),
                pltpu.SemaphoreType.DMA((5 * tp,)),
                pltpu.SemaphoreType.DMA((5 * tp,)),
                pltpu.SemaphoreType.DMA((tp * ep,)),
                pltpu.SemaphoreType.DMA((tp * ep,)),
                pltpu.SemaphoreType.DMA((tp * ep,)),
            ],
            compiler_params=pltpu.CompilerParams(collective_id=20, has_side_effects=True),
            name='gather',
        )(x, own.reshape(ir, 128))
        info = info.reshape(n_tok, 2 * top)

        loc = info[:, :top].astype(jnp.int32) - j * e_loc
        ga = info[:, top:]
        ids = jnp.arange(e_loc, dtype=jnp.int32)
        hit = jnp.any(loc.T[None] == ids[:, None, None], axis=1)
        before = jnp.arange(n_half)[:, None] < jnp.arange(n_half)[None, :]
        hit2 = hit.reshape(e_loc * 2, n_half)
        pos = jnp.dot(hit2.astype(jnp.bfloat16), before.astype(jnp.bfloat16),
                      preferred_element_type=jnp.float32).astype(jnp.int32).reshape(e_loc, 2, n_half)
        n = jnp.sum(hit2.astype(jnp.int32), axis=1).reshape(e_loc, 2)
        off = jnp.sum(jnp.where(ids[:, None, None] > ids[None, :, None], n[None], 0), axis=1)
        total = jnp.sum(n, axis=0)
        lead = off % 8
        nb = jnp.where(n > 0, (lead + n + 7) // 8, 0)
        left = jnp.broadcast_to(jnp.where(total % 8 > 0, total // 8, -1)[None], (e_loc, 2))
        meta = jnp.concatenate([nb, off // 8, (off + n) % 8, left], axis=1)
        base = jnp.stack([lead[:, 0], nb[:, 0] * 8 + lead[:, 1]], axis=1)
        dest = jnp.where(hit, (base[:, :, None] + pos).reshape(e_loc, n_tok), -1)

        full = -(-n_half * top // TC) * TC
        part = pl.pallas_call(
            expert_kernel,
            grid_spec=pltpu.PrefetchScalarGridSpec(
                num_scalar_prefetch=1,
                grid=(e_loc,),
                in_specs=[
                    pl.BlockSpec((e_loc, 1, n_tok), lambda e, m: (0, 0, 0)),
                    pl.BlockSpec((n_tok, d), lambda e, m: (0, 0)),
                    pl.BlockSpec((1, d, f), lambda e, m: (e, 0, 0)),
                    pl.BlockSpec((1, d, f), lambda e, m: (e, 0, 0)),
                    pl.BlockSpec((1, f, d), lambda e, m: (e, 0, 0)),
                ],
                out_specs=pl.BlockSpec(memory_space=pl.ANY),
                scratch_shapes=[
                    pltpu.VMEM((2, TM, d), jnp.float32),
                    pltpu.VMEM((2, 8, d), jnp.float32),
                    pltpu.VMEM((2, TM, d), x.dtype),
                    pltpu.SMEM((4,), jnp.int32),
                    pltpu.SemaphoreType.DMA((2,)),
                ]),
            out_shape=jax.ShapeDtypeStruct((2, full, d), jnp.float32),
            compiler_params=pltpu.CompilerParams(dimension_semantics=('arbitrary',), vmem_limit_bytes=60000 * 1024),
            name='experts',
        )(meta, dest.reshape(e_loc, 1, n_tok), xa, w1, w3, w2)

        row = (off[:, :, None] + pos)[:, side]
        mine = loc.reshape(2, n_half, top)[side]
        same = mine[:, :, None] == ids[None, None, :]
        rows = jnp.sum(jnp.where(same, row.T[:, None, :], 0), axis=2)
        rows = jnp.where(jnp.any(same, axis=2), rows, -1)
        order = lambda v: v.reshape(tp // 2, ep, t_loc, top).transpose(1, 0, 2, 3).reshape(n_half, top)

        def chain(size, ident):
            return pl.pallas_call(
                functools.partial(chain_kernel, tp, size // BR),
                in_specs=[pl.BlockSpec(memory_space=pltpu.SMEM), vmem, vmem, any_],
                out_specs=vmem,
                out_shape=jax.ShapeDtypeStruct((n_half, d), jnp.float32),
                scratch_shapes=[
                    pltpu.VMEM((2, NO, BR, d), jnp.float32),
                    pltpu.VMEM((2, NS, BR, d), jnp.float32),
                    pltpu.VMEM((2, NS, BR, d), jnp.float32),
                    pltpu.VMEM((TC, d), jnp.bfloat16),
                    pltpu.SemaphoreType.DMA((2, NO)),
                    pltpu.SemaphoreType.DMA((2, NS)),
                    pltpu.SemaphoreType.DMA((2, NS)),
                    pltpu.SemaphoreType.REGULAR((2,)),
                ],
                compiler_params=pltpu.CompilerParams(collective_id=ident, has_side_effects=True, vmem_limit_bytes=60000 * 1024),
                name=f'chain{size}',
            )

        sizes = tuple(s for s in SIZES if s < full) + (full,)
        need = jnp.max(total)
        which = jnp.sum((need > jnp.array(sizes[:-1], jnp.int32)).astype(jnp.int32))
        py = lax.switch(which, [chain(s, i + 1) for i, s in enumerate(sizes)],
                        total[side].reshape(1), order(rows), order(ga.reshape(2, n_half, top)[side]), part)

        return pl.pallas_call(
            functools.partial(finish_kernel, tp),
            in_specs=[vmem],
            out_specs=vmem,
            out_shape=jax.ShapeDtypeStruct((t_loc, d), x.dtype),
            scratch_shapes=[
                pltpu.VMEM((2, 2 * t_loc, d), jnp.float32),
                pltpu.VMEM((2 * t_loc, d), jnp.float32),
                pltpu.VMEM((2 * t_loc, d), jnp.float32),
                pltpu.VMEM((2, t_loc // 2, d), x.dtype),
                pltpu.VMEM((2, t_loc // 2, d), x.dtype),
                pltpu.SemaphoreType.DMA((4, 2)),
                pltpu.SemaphoreType.DMA((4, 2)),
                pltpu.SemaphoreType.DMA((4,)),
                pltpu.SemaphoreType.DMA((4,)),
                pltpu.SemaphoreType.DMA((2,)),
                pltpu.SemaphoreType.DMA((2,)),
            ],
            compiler_params=pltpu.CompilerParams(collective_id=21, has_side_effects=True, vmem_limit_bytes=60000 * 1024),
            name='finish',
        )(py.reshape(ep, n_half // ep, d))

    return jax.shard_map(local, mesh=mesh,
                         in_specs=(tok_spec, tok_spec, tok_spec, P('ep', None, 'tp'), P('ep', None, 'tp'), P('ep', 'tp', None)),
                         out_specs=tok_spec, check_vma=False)
```
